32 devices in a mesh: pts: 16 (over z, y, x), grp: 2 (over core).
Axes of the slice: x: 2, y: 2, z: 4, core: 2. Of those that a mesh axis runs over, the one named last changes fastest.
Arguments:
- cam_jac: float32 [18, 262144], P(None, ('pts', 'grp')), may hold values from -0.25 to 0.25
- pt_jac: float32 [6, 262144], P(None, ('pts', 'grp')), may hold values from -6 to 6
- resid: float32 [2, 262144], P(None, ('pts', 'grp')), may hold values from -102 to 102
- obs_point: int32 [262144], P(('pts', 'grp')), may hold values from 0 to 65535, as said below
- obs_camera: int32 [262144], P(('pts', 'grp')), may hold values from 0 to 511
- camera_slot: int32 [512], replicated, may hold values from 0 to 511, each once
Outputs:
- cam_inverse: float32 [81, 512], P(None, ('pts', 'grp'))
- precond: float32 [9, 262144], P(None, ('pts', 'grp'))
The draws below stay inside these ranges and needn't reach their ends.
Inputs may be any that keep to these rules, and one draw needn't show every extreme that they name: `obs_point`: observation o names a point of block o // 8192, from (o // 8192) * 2048 to (o // 8192 + 1) * 2048 - 1; within each block of 8192 observations the point number never falls and rises by at most 1 from one observation to the next, and the block's first observation names the block's first point. Each slot appears once; camera c is owned by device camera_slot[c] // 16 of the joined axes pts+grp.
All inputs are finite; a program needn't handle non-finite values.
Results may differ from the reference program's by a relative error of at most 0.0003.
Values sent between devices are 32-bit elements; how exact they have to be, the bound alone decides.
No kernel may reach another device: no remote copies, remote signals or barrier semaphores. Data moves between devices by JAX's collectives and lax.ppermute only.
A program may use at most 64 MiB of HBM per device.

```python
import math
import jax
import jax.numpy as jnp
import numpy as np
from jax import lax

OBS_DEV = 8192
CAM_DEV = 16
PTS_DEV = 2048
OBS = 262144
CAMS = 512
N_PTS = 16
N_GRP = 2


def draw_obs_point(key, part):
    devices = OBS // OBS_DEV
    coins = jax.random.randint(jax.random.fold_in(key, 17), (devices, OBS_DEV), 0, 3, dtype=jnp.int32)
    rises = (coins == 0).astype(jnp.int32)
    rises = rises.at[:, 0].set(0)
    local = jnp.minimum(jnp.cumsum(rises, axis=1), PTS_DEV - 1).astype(jnp.int32)
    owner = jnp.arange(devices, dtype=jnp.int32)[:, None] * PTS_DEV
    return (owner + local).reshape(OBS).astype(jnp.int32)


def set_ends(values, rng, low, top_value):
    place = [jax.random.randint(jax.random.fold_in(rng, axis), (), 0, length) for axis, length in enumerate(values.shape)]
    longest = values.shape.index(max(values.shape))
    beside = place[:longest] + [(place[longest] + 1) % values.shape[longest]] + place[longest + 1:]
    return values.at[tuple(place)].set(low).at[tuple(beside)].set(top_value)


def levels(stream_key, dims, shards, smallest, high):
    level, own = 1.0, jax.random.fold_in(stream_key, 6)
    for dim, parts in shards:
        steps = jnp.exp(jax.random.uniform(jax.random.fold_in(own, dim), (parts,), jnp.float32, smallest / len(shards), high / len(shards)))
        level = level * jnp.repeat(steps, dims[dim] // parts).reshape([-1 if axis == dim else 1 for axis in range(len(dims))])
    return level


def cumulative_ranks(amount, skew):
    weights = [(1 << 20) // math.isqrt(standing ** skew) + 1 for standing in range(1, amount + 1)]
    width = 1 + sum(weights) // (1 << 30)
    return np.cumsum(np.array([max(1, weight // width) for weight in weights]))


def ranked_ids(stream_key, shape, amount, lean):
    table = cumulative_ranks(amount, lean)
    ticket = jax.random.randint(jax.random.fold_in(stream_key, 1), shape, 0, int(table[amount - 1]))
    standing = jnp.searchsorted(jnp.asarray(table, jnp.int32), ticket, side="right")
    return jax.random.permutation(jax.random.fold_in(stream_key, 2), amount)[standing].astype(jnp.int32)


def normal_values(stream_key, dims, width, bound, shards=(), kind=jnp.bfloat16):
    drawn = jax.random.normal(stream_key, dims, jnp.float32) * width
    if len(shards) > 0:
        drawn = levels(stream_key, dims, shards, -0.22, 0.18) * drawn
    return jnp.clip(drawn, min=-bound, max=bound).astype(kind)


def setup_inputs(seed: int = 0) -> dict:
    key_of = jax.random.split(jax.random.key(seed), 7)
    return {
        "cam_jac": normal_values(key_of[0], (18, OBS), (OBS_DEV // CAM_DEV) ** -0.5, 0.25, ((1, 32),), jnp.float32),
        "pt_jac": normal_values(key_of[1], (6, OBS), 1.0, 6.0, ((1, 32),), jnp.float32),
        "resid": normal_values(key_of[2], (2, OBS), (OBS_DEV // CAM_DEV // 32 + 1), 102.0, ((1, 32),), jnp.float32),
        "obs_point": draw_obs_point(jax.random.fold_in(key_of[6], 71), 0),
        "obs_camera": set_ends(ranked_ids(key_of[4], (OBS,), CAMS, 1), jax.random.fold_in(key_of[4], 3), 0, CAMS - 1).astype(jnp.int32),
        "camera_slot": jax.random.permutation(key_of[5], CAMS).astype(jnp.int32),
    }


DAMP = 1.0

def lower_pairs():
    return [(row_at, col_at) for row_at in range(9) for col_at in range(row_at + 1)]

def point_table(pt_jac, resid, local_point, npoints):
    entries = []
    for row_at in range(3):
        for col_at in range(row_at, 3):
            entries.append(pt_jac[row_at] * pt_jac[col_at] + pt_jac[3 + row_at] * pt_jac[3 + col_at])
    for row_at in range(3):
        entries.append(pt_jac[row_at] * resid[0] + pt_jac[3 + row_at] * resid[1])
    stacked = jnp.stack(entries, 0)
    sums = jnp.zeros((9, npoints), jnp.float32).at[:, local_point].add(stacked)
    v00 = sums[0] + DAMP
    v01 = sums[1]
    v02 = sums[2]
    v11 = sums[3] + DAMP
    v12 = sums[4]
    v22 = sums[5] + DAMP
    c00 = v11 * v22 - v12 * v12
    c01 = v02 * v12 - v01 * v22
    c02 = v01 * v12 - v02 * v11
    c11 = v00 * v22 - v02 * v02
    c12 = v01 * v02 - v00 * v12
    c22 = v00 * v11 - v01 * v01
    determ = v00 * c00 + v01 * c01 + v02 * c02
    i00 = c00 / determ
    i01 = c01 / determ
    i02 = c02 / determ
    i11 = c11 / determ
    i12 = c12 / determ
    i22 = c22 / determ
    w_zero = i00 * sums[6] + i01 * sums[7] + i02 * sums[8]
    w_one = i01 * sums[6] + i11 * sums[7] + i12 * sums[8]
    w_two = i02 * sums[6] + i12 * sums[7] + i22 * sums[8]
    table = jnp.stack([i00, i01, i02, i11, i12, i22, w_zero, w_one, w_two], 0)
    return table[:, local_point]

def obs_terms(cam_jac, pt_jac, resid, point_rows, pairs):
    i00, i01, i02, i11, i12, i22 = [point_rows[pos] for pos in range(6)]
    weights = [point_rows[6], point_rows[7], point_rows[8]]
    vinv = ((i00, i01, i02), (i01, i11, i12), (i02, i12, i22))
    prow = [[pt_jac[3 * rowp + inner] for inner in range(3)] for rowp in range(2)]
    usage = [[vinv[outer][0] * prow[rowp][0] + vinv[outer][1] * prow[rowp][1] + vinv[outer][2] * prow[rowp][2] for outer in range(3)] for rowp in range(2)]
    proj_zz = prow[0][0] * usage[0][0] + prow[0][1] * usage[0][1] + prow[0][2] * usage[0][2]
    proj_zo = prow[0][0] * usage[1][0] + prow[0][1] * usage[1][1] + prow[0][2] * usage[1][2]
    proj_oo = prow[1][0] * usage[1][0] + prow[1][1] * usage[1][1] + prow[1][2] * usage[1][2]
    keep = ((1.0 - proj_zz, -proj_zo), (-proj_zo, 1.0 - proj_oo))
    shifted = [resid[rowp] - (prow[rowp][0] * weights[0] + prow[rowp][1] * weights[1] + prow[rowp][2] * weights[2]) for rowp in range(2)]
    reduced = jnp.stack([cam_jac[col_at] * shifted[0] + cam_jac[9 + col_at] * shifted[1] for col_at in range(9)], 0)
    mixed = [[keep[rowp][0] * cam_jac[col_at] + keep[rowp][1] * cam_jac[9 + col_at] for col_at in range(9)] for rowp in range(2)]
    terms = jnp.stack([cam_jac[row_at] * mixed[0][col_at] + cam_jac[9 + row_at] * mixed[1][col_at] for row_at, col_at in pairs], 0)
    return (terms, reduced)

def chol_inverse(rows, pairs):
    entry = {pair: rows[pos] for pos, pair in enumerate(pairs)}
    factor = {}
    for col_at in range(9):
        diag = entry[col_at, col_at] + DAMP
        for inner in range(col_at):
            diag = diag - factor[col_at, inner] * factor[col_at, inner]
        root = jnp.sqrt(diag)
        factor[col_at, col_at] = root
        for row_at in range(col_at + 1, 9):
            value = entry[row_at, col_at]
            for inner in range(col_at):
                value = value - factor[row_at, inner] * factor[col_at, inner]
            factor[row_at, col_at] = value / root
    solved = {}
    for col_at in range(9):
        solved[col_at, col_at] = 1.0 / factor[col_at, col_at]
        for row_at in range(col_at + 1, 9):
            value = factor[row_at, col_at] * solved[col_at, col_at]
            for inner in range(col_at + 1, row_at):
                value = value + factor[row_at, inner] * solved[inner, col_at]
            solved[row_at, col_at] = -value / factor[row_at, row_at]
    result = {}
    for row_at in range(9):
        for col_at in range(row_at + 1):
            value = solved[row_at, row_at] * solved[row_at, col_at]
            for inner in range(row_at + 1, 9):
                value = value + solved[inner, row_at] * solved[inner, col_at]
            result[row_at, col_at] = value
            result[col_at, row_at] = value
    return jnp.stack([result[row_at, col_at] for row_at in range(9) for col_at in range(9)], 0)

def apply_inverse(picked, reduced, locate):
    outputs = []
    for row_at in range(9):
        value = picked[locate[row_at, 0]] * reduced[0]
        for col_at in range(1, 9):
            value = value + picked[locate[row_at, col_at]] * reduced[col_at]
        outputs.append(value)
    return jnp.stack(outputs, 0)

def reference(cam_jac, pt_jac, resid, obs_point, obs_camera, camera_slot):
    pairs = lower_pairs()
    devices = N_PTS * N_GRP

    def blocks(array):
        return jnp.moveaxis(array.reshape(array.shape[0], devices, OBS_DEV), 1, 0)
    slot = camera_slot[obs_camera]
    offsets = jnp.arange(devices, dtype=jnp.int32) * PTS_DEV

    def one_block(total, inputs):
        cam_part, pt_part, res_part, point_part, slot_part, offset = inputs
        rows = point_table(pt_part, res_part, point_part - offset, PTS_DEV)
        terms, reduced = obs_terms(cam_part, pt_part, res_part, rows, pairs)
        return (total.at[:, slot_part].add(terms), reduced)
    total, reduced = lax.scan(one_block, jnp.zeros((len(pairs), CAMS), jnp.float32), (blocks(cam_jac), blocks(pt_jac), blocks(resid), obs_point.reshape(devices, OBS_DEV), slot.reshape(devices, OBS_DEV), offsets))
    inverse = chol_inverse(total, pairs)
    locate = {(row_at, col_at): row_at * 9 + col_at for row_at in range(9) for col_at in range(9)}

    def finish(inputs):
        slot_part, reduced_part = inputs
        return apply_inverse(inverse[:, slot_part], reduced_part, locate)
    precond = lax.map(finish, (slot.reshape(devices, OBS_DEV), reduced))
    precond = jnp.moveaxis(precond, 0, 1).reshape(9, OBS)
    return (inverse, precond)
```

```python
import functools

import jax
import jax.numpy as jnp
from jax import lax
from jax.experimental import pallas as pl
from jax.experimental.pallas import tpu as pltpu
from jax.sharding import PartitionSpec as P

AXES = ("pts", "grp")
DAMP = 1.0
LANES = 128
ROWS = 48
GROUP = 8


def split3(value):
    high = value.astype(jnp.bfloat16)
    rest = value - high.astype(jnp.float32)
    mid = rest.astype(jnp.bfloat16)
    low = (rest - mid.astype(jnp.float32)).astype(jnp.bfloat16)
    return high, mid, low


def dot_nn(left, right):
    return lax.dot_general(left, right, (((1,), (0,)), ((), ())), preferred_element_type=jnp.float32)


def dot_nt(left, right):
    return lax.dot_general(left, right, (((1,), (1,)), ((), ())), preferred_element_type=jnp.float32)


def row_of(row_at, col_at):
    if row_at == 8 and col_at == 8:
        return 36
    if row_at == 8:
        return 40 + col_at
    if col_at == 8:
        return 40 + row_at
    gap = (col_at - row_at) % 8
    if gap > 4 or (gap == 4 and row_at >= 4):
        return 8 * ((row_at - col_at) % 8) + col_at
    return 8 * gap + row_at


def one_hot(named, first, count):
    rows = lax.broadcasted_iota(jnp.int32, (16, LANES), 0) + first
    gap = (jnp.broadcast_to(named, (16, LANES)) - rows).astype(jnp.int16)
    one = jnp.ones((16, LANES), jnp.bfloat16)
    zero = jnp.zeros((16, LANES), jnp.bfloat16)
    return jnp.concatenate(
        [jnp.where(gap == jnp.int16(16 * at), one, zero) for at in range(count // 16)], 0
    )


def gather_terms_kernel(
    base_ref, pt_ref, res_ref, point_ref, cam_ref, named_ref,
    part_ref, red_ref, last_ref,
    dense_ref, total_ref, keep_ref, acc_ref, where_ref,
):
    tiles = point_ref.shape[0]
    half = part_ref.shape[2]
    row = lax.broadcasted_iota(jnp.int32, (8, LANES), 0)
    first_point = point_ref[0:1, 0:1]
    where_ref[...] = (point_ref[...] - first_point).astype(jnp.float32)

    def sums(step, carry):
        start = pl.multiple_of(step * GROUP, GROUP)
        lane = pl.multiple_of(step * (GROUP * LANES), GROUP * LANES)
        points = where_ref[pl.ds(start, GROUP), :]
        columns = jnp.transpose(points)
        for at in range(GROUP):
            here = pl.ds(lane + at * LANES, LANES)
            value = jnp.concatenate([pt_ref[:, here], res_ref[:, here]], 0)
            shift1 = pltpu.roll(value, 7, 0)
            shift2 = pltpu.roll(value, 6, 0)
            error = jnp.where(row < 3, value[6:7], value[7:8])

            def both(prod):
                return prod + pltpu.roll(prod, 5, 0)

            upper = jnp.where(
                row < 3,
                both(value * value),
                jnp.where(
                    row < 5,
                    pltpu.roll(both(value * shift1), 3, 0),
                    pltpu.roll(both(value * shift2), 5, 0),
                ),
            )
            lower = both(value * error)
            left = jnp.concatenate(split3(jnp.concatenate([upper, lower], 0)), 0)
            same = jnp.where(
                jnp.broadcast_to(columns[:, at : at + 1], (LANES, LANES))
                == jnp.broadcast_to(points[at : at + 1], (LANES, LANES)),
                1.0,
                0.0,
            ).astype(jnp.bfloat16)
            found = dot_nn(left, same)
            found = found[0:16] + found[16:32] + found[32:48]
            total_ref[pl.ds(start + at, 8, stride=tiles), :] = found[0:8]
            total_ref[pl.ds(8 * tiles + start + at, 8, stride=tiles), :] = found[8:16]
            dense_ref[pl.ds(start + at, 8, stride=tiles), :] = value
        return carry

    lax.fori_loop(0, tiles // GROUP, sums, 0)

    places = where_ref[...]
    turned = jnp.transpose(places)
    tile_at = lax.broadcasted_iota(jnp.int32, (tiles, tiles), 0)
    other = lax.broadcasted_iota(jnp.int32, (tiles, tiles), 1)
    before = jnp.where((other < tile_at) & (turned[LANES - 1 : LANES, :] == places[:, 0:1]), 1.0, 0.0)
    after = jnp.where((other > tile_at) & (turned[0:1, :] == places[:, LANES - 1 : LANES]), 1.0, 0.0)
    entries = (0, 1, 2, 3, 4, 5, 8, 9, 10)
    lane_at = lax.broadcasted_iota(jnp.int32, (tiles, LANES), 1)
    heads = jnp.zeros((tiles, LANES), jnp.float32)
    tails = jnp.zeros((tiles, LANES), jnp.float32)
    for pos in entries:
        found = total_ref[pos * tiles : (pos + 1) * tiles, :]
        heads = jnp.where(lane_at == pos, found[:, 0:1], heads)
        tails = jnp.where(lane_at == pos, found[:, LANES - 1 : LANES], tails)

    def carried(matrix, column):
        parts = [dot_nn(matrix.astype(jnp.bfloat16), part) for part in split3(column)]
        return parts[0] + parts[1] + parts[2]

    from_before = carried(before, tails)
    from_after = carried(after, heads)

    for start in range(0, tiles, 8):
        place = places[start : start + 8]
        is_head = place == place[:, 0:1]
        is_tail = place == place[:, LANES - 1 : LANES]
        add_before = from_before[start : start + 8]
        add_after = from_after[start : start + 8]

        def total(pos):
            value = total_ref[pos * tiles + start : pos * tiles + start + 8, :]
            value = value + jnp.where(is_head, add_before[:, pos : pos + 1], 0.0)
            return value + jnp.where(is_tail, add_after[:, pos : pos + 1], 0.0)

        v00, v11, v22 = [total(pos) + DAMP for pos in (0, 1, 2)]
        v01, v12, v02 = [total(pos) for pos in (3, 4, 5)]
        bees = [total(pos) for pos in (8, 9, 10)]
        dense = [dense_ref[pos * tiles + start : pos * tiles + start + 8, :] for pos in range(8)]
        c00 = v11 * v22 - v12 * v12
        c01 = v02 * v12 - v01 * v22
        c02 = v01 * v12 - v02 * v11
        c11 = v00 * v22 - v02 * v02
        c12 = v01 * v02 - v00 * v12
        c22 = v00 * v11 - v01 * v01
        scale = 1.0 / (v00 * c00 + v01 * c01 + v02 * c02)
        vinv = [[c00 * scale, c01 * scale, c02 * scale]]
        vinv.append([vinv[0][1], c11 * scale, c12 * scale])
        vinv.append([vinv[0][2], vinv[1][2], c22 * scale])

        def times(vec):
            return [vinv[at][0] * vec[0] + vinv[at][1] * vec[1] + vinv[at][2] * vec[2] for at in range(3)]

        def inner(left, right):
            return left[0] * right[0] + left[1] * right[1] + left[2] * right[2]

        top, low = dense[0:3], dense[3:6]
        use_top, use_low, weight = times(top), times(low), times(bees)
        results = (
            1.0 - inner(top, use_top),
            -inner(top, use_low),
            1.0 - inner(low, use_low),
            dense[6] - inner(top, weight),
            dense[7] - inner(low, weight),
        )
        for pos, value in enumerate(results):
            keep_ref[pos * tiles + start : pos * tiles + start + 8, :] = value

    acc_ref[...] = jnp.zeros(acc_ref.shape, jnp.float32)

    def scatter(step, carry):
        start = pl.multiple_of(step * GROUP, GROUP)
        lane = pl.multiple_of(step * (GROUP * LANES), GROUP * LANES)
        lefts = []
        rights = []
        for at in range(GROUP):
            here = pl.ds(lane + at * LANES, LANES)

            def spread(pos):
                return jnp.broadcast_to(keep_ref[pl.ds(pos * tiles + start + at, 1), :], (8, LANES))

            k00, k01, k11, s0, s1 = [spread(pos) for pos in range(5)]
            zero, one = cam_ref[0:8, here], cam_ref[9:17, here]
            zero8 = jnp.broadcast_to(cam_ref[8:9, here], (8, LANES))
            one8 = jnp.broadcast_to(cam_ref[17:18, here], (8, LANES))
            m0 = k00 * zero + k01 * one
            m1 = k01 * zero + k11 * one
            corner = zero8 * (k00 * zero8 + k01 * one8) + one8 * (k01 * zero8 + k11 * one8)
            pieces = [zero * m0 + one * m1]
            for gap in range(1, 5):
                pieces.append(zero * pltpu.roll(m0, 8 - gap, 0) + one * pltpu.roll(m1, 8 - gap, 0))
            pieces[4] = jnp.where(row == 4, corner, pieces[4])
            pieces.append(zero8 * m0 + one8 * m1)
            lefts.append(jnp.concatenate(split3(jnp.concatenate(pieces, 0)), 0))
            red_ref[:, here] = zero * s0 + one * s1
            last_ref[pl.ds(start + at, 1), :] = (zero8 * s0 + one8 * s1)[0:1]
            named = named_ref[pl.ds(start + at, 1), :]
            rights.append(
                jnp.concatenate([one_hot(named, base_ref[0], half), one_hot(named, base_ref[1], half)], 0)
            )
        acc_ref[...] += dot_nt(jnp.concatenate(lefts, 1), jnp.concatenate(rights, 1))
        return carry

    lax.fori_loop(0, tiles // GROUP, scatter, 0)
    done = acc_ref[0:ROWS, :] + acc_ref[ROWS : 2 * ROWS, :] + acc_ref[2 * ROWS : 3 * ROWS, :]
    part_ref[0] = done[:, 0:half]
    part_ref[1] = done[:, half : 2 * half]


def inverse_of(entry):
    entry = dict(entry)
    root = {}
    factor = {}
    for col_at in range(9):
        root[col_at] = lax.rsqrt(entry[col_at, col_at])
        for row_at in range(col_at + 1, 9):
            factor[row_at, col_at] = entry[row_at, col_at] * root[col_at]
        for row_at in range(col_at + 1, 9):
            for inner in range(col_at + 1, row_at + 1):
                entry[row_at, inner] = entry[row_at, inner] - factor[row_at, col_at] * factor[inner, col_at]
    solved = {}
    for col_at in range(9):
        solved[col_at, col_at] = root[col_at]
        for row_at in range(col_at + 1, 9):
            value = factor[row_at, col_at] * solved[col_at, col_at]
            for inner in range(col_at + 1, row_at):
                value = value + factor[row_at, inner] * solved[inner, col_at]
            solved[row_at, col_at] = -value * root[row_at]
    result = {}
    for row_at in range(9):
        for col_at in range(row_at + 1):
            value = solved[row_at, row_at] * solved[row_at, col_at]
            for inner in range(row_at + 1, 9):
                value = value + solved[inner, row_at] * solved[inner, col_at]
            result[row_at, col_at] = value
    return result


def apply_kernel(
    base_ref, mine_ref, theirs_ref, slot_ref, named_ref, red_ref, last_ref,
    inv_ref, out_ref,
    entry_ref, table_ref,
):
    tiles = named_ref.shape[0]
    half = mine_ref.shape[1]
    owned = inv_ref.shape[1]
    cols = 2 * half // LANES
    row = lax.broadcasted_iota(jnp.int32, (8, LANES), 0)
    step_rows = entry_ref.shape[0] // ROWS
    for block in range(ROWS // 8):
        for col in range(cols):
            source = mine_ref if col < cols // 2 else theirs_ref
            at = (col % (cols // 2)) * LANES
            entry_ref[pl.ds(block * 8 * step_rows + col, 8, stride=step_rows), :] = source[
                block * 8 : block * 8 + 8, at : at + LANES
            ]

    def entry_at(row_at, col_at):
        at = row_of(row_at, col_at) * step_rows
        return entry_ref[at : at + cols, :]

    entry = {(r, c): entry_at(r, c) for r in range(9) for c in range(r + 1)}
    for at in range(9):
        entry[at, at] = entry[at, at] + DAMP
    result = inverse_of(entry)
    entry_ref[...] = jnp.zeros(entry_ref.shape, jnp.float32)
    for (row_at, col_at), value in result.items():
        at = row_of(row_at, col_at) * step_rows
        entry_ref[at : at + cols, :] = value
    for col in range(cols):
        blocks = [
            entry_ref[pl.ds(block * 8 * step_rows + col, 8, stride=step_rows), :] for block in range(ROWS // 8)
        ]
        table_ref[:, col * LANES : (col + 1) * LANES] = jnp.concatenate(
            split3(jnp.concatenate(blocks, 0)), 0
        )

    want = lax.broadcasted_iota(jnp.int32, (LANES, half), 0) + base_ref[2]
    picks = [
        jnp.where((slot_ref[at : at + 1, :] == want), 1.0, 0.0).astype(jnp.bfloat16) for at in range(2)
    ]
    own = dot_nt(table_ref[...], jnp.concatenate(picks, 1))
    own = own[0:ROWS] + own[ROWS : 2 * ROWS] + own[2 * ROWS : 3 * ROWS]
    for row_at in range(9):
        for col_at in range(9):
            at = row_of(row_at, col_at)
            inv_ref[row_at * 9 + col_at : row_at * 9 + col_at + 1, :] = own[at : at + 1, 0:owned]

    def pick(step, carry):
        start = pl.multiple_of(step * GROUP, GROUP)
        lane = pl.multiple_of(step * (GROUP * LANES), GROUP * LANES)
        rights = []
        for at in range(GROUP):
            named = named_ref[pl.ds(start + at, 1), :]
            rights.append(
                jnp.concatenate([one_hot(named, base_ref[0], half), one_hot(named, base_ref[1], half)], 0)
            )
        found = dot_nn(table_ref[...], jnp.concatenate(rights, 1))
        found = found[0:ROWS] + found[ROWS : 2 * ROWS] + found[2 * ROWS : 3 * ROWS]
        for at in range(GROUP):
            here = pl.ds(lane + at * LANES, LANES)
            block = [found[8 * pos : 8 * pos + 8, at * LANES : (at + 1) * LANES] for pos in range(6)]
            red = red_ref[:, here]
            last = jnp.broadcast_to(last_ref[pl.ds(start + at, 1), :], (8, LANES))
            whole = jnp.where(row < 4, block[4], pltpu.roll(block[4], 4, 0))
            value = block[0] * red + block[5] * last + whole * pltpu.roll(red, 4, 0)
            for gap in range(1, 4):
                value = value + block[gap] * pltpu.roll(red, 8 - gap, 0)
                value = value + pltpu.roll(block[gap] * red, gap, 0)
            out_ref[0:8, here] = value
            edge = jnp.sum(block[5] * red, axis=0, keepdims=True)
            out_ref[8:9, here] = edge + (block[4] * last)[4:5]
        return carry

    lax.fori_loop(0, tiles // GROUP, pick, 0)


def flips(count, mask):
    return [(at, at ^ mask) for at in range(count)]


def shards(cam_jac, pt_jac, resid, obs_point, obs_camera, camera_slot, *, npts, ngrp):
    count = npts * ngrp
    cams = camera_slot.shape[0]
    half = cams // 2
    owned = cams // count
    size = obs_point.shape[0]
    tiles = size // LANES
    grp = lax.axis_index("grp")
    device = lax.axis_index(AXES)
    base = jnp.stack([grp * half, (1 - grp) * half, device * owned]).astype(jnp.int32)
    named = obs_camera.reshape(tiles, LANES)
    smem = pl.BlockSpec(memory_space=pltpu.SMEM)
    vmem = pl.BlockSpec(memory_space=pltpu.VMEM)
    part, red, last = pl.pallas_call(
        gather_terms_kernel,
        in_specs=[smem] + [vmem] * 5,
        out_specs=[vmem] * 3,
        out_shape=[
            jax.ShapeDtypeStruct((2, ROWS, half), jnp.float32),
            jax.ShapeDtypeStruct((8, size), jnp.float32),
            jax.ShapeDtypeStruct((tiles, LANES), jnp.float32),
        ],
        scratch_shapes=[
            pltpu.VMEM((8 * tiles, LANES), jnp.float32),
            pltpu.VMEM((16 * tiles, LANES), jnp.float32),
            pltpu.VMEM((5 * tiles, LANES), jnp.float32),
            pltpu.VMEM((3 * ROWS, cams), jnp.float32),
            pltpu.VMEM((tiles, LANES), jnp.float32),
        ],
        name="terms",
    )(base, pt_jac, resid, obs_point.reshape(tiles, LANES), cam_jac, named)

    total = part[0] + lax.ppermute(part[1], AXES, flips(count, 1))
    bit = ngrp
    while bit < count:
        masks = (bit, 2 * bit, 3 * bit) if 2 * bit < count else (bit,)
        got = [lax.ppermute(total, AXES, flips(count, mask)) for mask in masks]
        for value in got:
            total = total + value
        bit *= 4
    theirs = lax.ppermute(total, AXES, flips(count, 1))

    slots = camera_slot.reshape(2, half)
    slots = jnp.where(grp == 0, slots, slots[::-1])
    inverse, precond = pl.pallas_call(
        apply_kernel,
        in_specs=[smem] + [vmem] * 6,
        out_specs=[vmem] * 2,
        out_shape=[
            jax.ShapeDtypeStruct((81, owned), jnp.float32),
            jax.ShapeDtypeStruct((9, size), jnp.float32),
        ],
        scratch_shapes=[
            pltpu.VMEM((ROWS * max(8, 2 * half // LANES), LANES), jnp.float32),
            pltpu.VMEM((3 * ROWS, cams), jnp.bfloat16),
        ],
        name="apply",
    )(base, total, theirs, slots, named, red, last)
    return (inverse, precond)


def solution(mesh):
    spread = P(None, AXES)
    in_specs = (spread, spread, spread, P(AXES), P(AXES), P())
    body = functools.partial(shards, npts=mesh.shape["pts"], ngrp=mesh.shape["grp"])
    return jax.shard_map(body, mesh=mesh, in_specs=in_specs, out_specs=(spread, spread), check_vma=False)
```

```python
import functools

import jax
import jax.numpy as jnp
from jax import lax
from jax.experimental import pallas as pl
from jax.experimental.pallas import tpu as pltpu
from jax.sharding import PartitionSpec as P

AXES = ("pts", "grp")
DAMP = 1.0
LANES = 128
ROWS = 48
GROUP = 8
SCATTER = 8


def split3(value):
    high = value.astype(jnp.bfloat16)
    rest = value - high.astype(jnp.float32)
    mid = rest.astype(jnp.bfloat16)
    low = (rest - mid.astype(jnp.float32)).astype(jnp.bfloat16)
    return high, mid, low


def dot_nn(left, right):
    return lax.dot_general(left, right, (((1,), (0,)), ((), ())), preferred_element_type=jnp.float32)


def dot_nt(left, right):
    return lax.dot_general(left, right, (((1,), (1,)), ((), ())), preferred_element_type=jnp.float32)


def row_of(row_at, col_at):
    if row_at == 8 and col_at == 8:
        return 36
    if row_at == 8:
        return 40 + col_at
    if col_at == 8:
        return 40 + row_at
    gap = (col_at - row_at) % 8
    if gap > 4 or (gap == 4 and row_at >= 4):
        return 8 * ((row_at - col_at) % 8) + col_at
    return 8 * gap + row_at


def other_half(named, grp, half):
    swapped = jnp.where(named < half, named + half, named - half)
    return jnp.where(grp == 0, named, swapped)


def terms_kernel(
    pt_ref, res_ref, point_ref, named_ref, cam_hbm,
    mine_ref, theirs_ref, red_ref, last_ref, place_ref,
    cam_ref, dense_ref, total_ref, keep_ref, where_ref, sem,
):
    tiles = point_ref.shape[0]
    half = mine_ref.shape[1]
    cams = 2 * half
    load = pltpu.make_async_copy(cam_hbm, cam_ref, sem)
    load.start()
    row = lax.broadcasted_iota(jnp.int32, (8, LANES), 0)
    where_ref[...] = (point_ref[...] - point_ref[0:1, 0:1]).astype(jnp.float32)
    place_ref[...] = other_half(named_ref[...], lax.axis_index("grp"), half)
    one = jnp.ones((LANES, LANES), jnp.bfloat16)
    zero_one = jnp.zeros((LANES, LANES), jnp.bfloat16)

    camera_columns = []
    for start in range(0, tiles, GROUP):
        points = where_ref[start : start + GROUP, :]
        both_ids = jnp.concatenate([points, place_ref[start : start + GROUP, :].astype(jnp.float32)], 0)
        columns = jnp.transpose(both_ids).astype(jnp.int32).astype(jnp.int16)
        camera_columns.append(columns)
        points = points.astype(jnp.int32)
        for at in range(GROUP):
            tile = start + at
            here = slice(tile * LANES, (tile + 1) * LANES)
            value = jnp.concatenate([pt_ref[:, here], res_ref[:, here]], 0)
            shift1 = pltpu.roll(value, 7, 0)
            shift2 = pltpu.roll(value, 6, 0)
            error = jnp.where(row < 3, value[6:7], value[7:8])

            def both(prod):
                return prod + pltpu.roll(prod, 5, 0)

            upper = jnp.where(
                row < 3,
                both(value * value),
                jnp.where(
                    row < 5,
                    pltpu.roll(both(value * shift1), 3, 0),
                    pltpu.roll(both(value * shift2), 5, 0),
                ),
            )
            lower = both(value * error)
            left = jnp.concatenate(split3(jnp.concatenate([upper, lower], 0)), 0)
            line = jnp.broadcast_to(points[at : at + 1], (16, LANES)).astype(jnp.int16)
            same = jnp.where(
                jnp.broadcast_to(columns[:, at : at + 1], (LANES, LANES)) == jnp.concatenate([line] * 8, 0),
                one,
                zero_one,
            )
            found = dot_nn(left, same)
            found = found[0:16] + found[16:32] + found[32:48]
            total_ref[pl.ds(tile, 8, stride=tiles), :] = found[0:8]
            total_ref[pl.ds(8 * tiles + tile, 8, stride=tiles), :] = found[8:16]
            dense_ref[pl.ds(tile, 8, stride=tiles), :] = value

    places = where_ref[...]
    turned = jnp.transpose(places)
    tile_at = lax.broadcasted_iota(jnp.int32, (tiles, tiles), 0)
    other = lax.broadcasted_iota(jnp.int32, (tiles, tiles), 1)
    before = jnp.where((other < tile_at) & (turned[LANES - 1 : LANES, :] == places[:, 0:1]), 1.0, 0.0)
    after = jnp.where((other > tile_at) & (turned[0:1, :] == places[:, LANES - 1 : LANES]), 1.0, 0.0)
    lane_at = lax.broadcasted_iota(jnp.int32, (tiles, LANES), 1)
    heads = jnp.zeros((tiles, LANES), jnp.float32)
    tails = jnp.zeros((tiles, LANES), jnp.float32)
    for pos in (0, 1, 2, 3, 4, 5, 8, 9, 10):
        found = total_ref[pos * tiles : (pos + 1) * tiles, :]
        heads = jnp.where(lane_at == pos, found[:, 0:1], heads)
        tails = jnp.where(lane_at == pos, found[:, LANES - 1 : LANES], tails)

    def carried(matrix, column):
        parts = [dot_nn(matrix.astype(jnp.bfloat16), part) for part in split3(column)]
        return parts[0] + parts[1] + parts[2]

    from_before = carried(before, tails)
    from_after = carried(after, heads)

    for start in range(0, tiles, 8):
        place = places[start : start + 8]
        is_head = place == place[:, 0:1]
        is_tail = place == place[:, LANES - 1 : LANES]
        add_before = from_before[start : start + 8]
        add_after = from_after[start : start + 8]

        def total(pos):
            value = total_ref[pos * tiles + start : pos * tiles + start + 8, :]
            value = value + jnp.where(is_head, add_before[:, pos : pos + 1], 0.0)
            return value + jnp.where(is_tail, add_after[:, pos : pos + 1], 0.0)

        v00, v11, v22 = [total(pos) + DAMP for pos in (0, 1, 2)]
        v01, v12, v02 = [total(pos) for pos in (3, 4, 5)]
        bees = [total(pos) for pos in (8, 9, 10)]
        dense = [dense_ref[pos * tiles + start : pos * tiles + start + 8, :] for pos in range(8)]
        c00 = v11 * v22 - v12 * v12
        c01 = v02 * v12 - v01 * v22
        c02 = v01 * v12 - v02 * v11
        c11 = v00 * v22 - v02 * v02
        c12 = v01 * v02 - v00 * v12
        c22 = v00 * v11 - v01 * v01
        scale = 1.0 / (v00 * c00 + v01 * c01 + v02 * c02)
        vinv = [[c00 * scale, c01 * scale, c02 * scale]]
        vinv.append([vinv[0][1], c11 * scale, c12 * scale])
        vinv.append([vinv[0][2], vinv[1][2], c22 * scale])

        def times(vec):
            return [vinv[at][0] * vec[0] + vinv[at][1] * vec[1] + vinv[at][2] * vec[2] for at in range(3)]

        def inner(left, right):
            return left[0] * right[0] + left[1] * right[1] + left[2] * right[2]

        top, low = dense[0:3], dense[3:6]
        use_top, use_low, weight = times(top), times(low), times(bees)
        results = (
            1.0 - inner(top, use_top),
            -inner(top, use_low),
            1.0 - inner(low, use_low),
            dense[6] - inner(top, weight),
            dense[7] - inner(low, weight),
        )
        for pos, value in enumerate(results):
            keep_ref[pos * tiles + start : pos * tiles + start + 8, :] = value

    load.wait()
    lane16 = lax.broadcasted_iota(jnp.int32, (16, LANES), 1)
    names = [(lane16 + at * LANES).astype(jnp.int16) for at in range(cams // LANES)]
    one = jnp.ones((16, LANES), jnp.bfloat16)
    zero_one = jnp.zeros((16, LANES), jnp.bfloat16)
    acc = jnp.zeros((3 * ROWS, cams), jnp.float32)
    for start in range(0, tiles, SCATTER):
        lefts = []
        rights = []
        for tile in range(start, start + SCATTER):
            here = slice(tile * LANES, (tile + 1) * LANES)

            def spread(ref, at):
                return ref[pl.ds(at, 8, stride=0), :]

            k00, k01, k11, s0, s1 = [spread(keep_ref, pos * tiles + tile) for pos in range(5)]
            zero, one_row = cam_ref[0:8, here], cam_ref[9:17, here]
            zero8 = jnp.broadcast_to(cam_ref[8:9, here], (8, LANES))
            one8 = jnp.broadcast_to(cam_ref[17:18, here], (8, LANES))
            m0 = k00 * zero + k01 * one_row
            m1 = k01 * zero + k11 * one_row
            corner = zero8 * (k00 * zero8 + k01 * one8) + one8 * (k01 * zero8 + k11 * one8)
            pieces = [zero * m0 + one_row * m1]
            for gap in range(1, 5):
                pieces.append(zero * pltpu.roll(m0, 8 - gap, 0) + one_row * pltpu.roll(m1, 8 - gap, 0))
            pieces[4] = jnp.where(row == 4, corner, pieces[4])
            pieces.append(zero8 * m0 + one8 * m1)
            lefts.append(jnp.concatenate(split3(jnp.concatenate(pieces, 0)), 0))
            red_ref[:, here] = zero * s0 + one_row * s1
            last_ref[tile : tile + 1, :] = (zero8 * s0 + one8 * s1)[0:1]
            source = camera_columns[tile // GROUP]
            lane = GROUP + tile % GROUP
            for at in range(0, LANES, 16):
                column = jnp.broadcast_to(source[at : at + 16, lane : lane + 1], (16, LANES))
                rights.append(jnp.concatenate([jnp.where(column == name, one, zero_one) for name in names], 1))
        acc = acc + dot_nn(jnp.concatenate(lefts, 1), jnp.concatenate(rights, 0))
    done = acc[0:ROWS] + acc[ROWS : 2 * ROWS] + acc[2 * ROWS : 3 * ROWS]
    mine_ref[...] = done[:, 0:half]
    theirs_ref[...] = done[:, half:cams]


def inverse_of(entry):
    entry = dict(entry)
    root = {}
    factor = {}
    for col_at in range(9):
        root[col_at] = lax.rsqrt(entry[col_at, col_at])
        for row_at in range(col_at + 1, 9):
            factor[row_at, col_at] = entry[row_at, col_at] * root[col_at]
        for row_at in range(col_at + 1, 9):
            for inner in range(col_at + 1, row_at + 1):
                entry[row_at, inner] = entry[row_at, inner] - factor[row_at, col_at] * factor[inner, col_at]
    solved = {}
    for col_at in range(9):
        solved[col_at, col_at] = root[col_at]
        for row_at in range(col_at + 1, 9):
            value = factor[row_at, col_at] * solved[col_at, col_at]
            for inner in range(col_at + 1, row_at):
                value = value + factor[row_at, inner] * solved[inner, col_at]
            solved[row_at, col_at] = -value * root[row_at]
    result = {}
    for row_at in range(9):
        for col_at in range(row_at + 1):
            value = solved[row_at, row_at] * solved[row_at, col_at]
            for inner in range(row_at + 1, 9):
                value = value + solved[inner, row_at] * solved[inner, col_at]
            result[row_at, col_at] = value
    return result


def apply_kernel(
    mine_ref, theirs_ref, place_ref, red_ref, last_ref, slot_ref,
    inv_ref, out_hbm,
    entry_ref, table_ref, own_ref, out_ref, sems,
):
    tiles = place_ref.shape[0]
    half = mine_ref.shape[1]
    cams = 2 * half
    owned = inv_ref.shape[0]
    cols = cams // LANES
    grp = lax.axis_index("grp")
    row = lax.broadcasted_iota(jnp.int32, (8, LANES), 0)
    step_rows = entry_ref.shape[0] // ROWS
    for block in range(ROWS // 8):
        for col in range(cols):
            source = mine_ref if col < cols // 2 else theirs_ref
            at = (col % (cols // 2)) * LANES
            entry_ref[pl.ds(block * 8 * step_rows + col, 8, stride=step_rows), :] = source[
                block * 8 : block * 8 + 8, at : at + LANES
            ]

    def entry_at(row_at, col_at):
        at = row_of(row_at, col_at) * step_rows
        return entry_ref[at : at + cols, :]

    entry = {(r, c): entry_at(r, c) for r in range(9) for c in range(r + 1)}
    for at in range(9):
        entry[at, at] = entry[at, at] + DAMP
    result = inverse_of(entry)
    spare = jnp.zeros((cols, LANES), jnp.float32)
    for at in (37, 38, 39):
        entry_ref[at * step_rows : at * step_rows + cols, :] = spare
    for (row_at, col_at), value in result.items():
        at = row_of(row_at, col_at) * step_rows
        entry_ref[at : at + cols, :] = value
    tables = []
    for col in range(cols):
        blocks = [
            entry_ref[pl.ds(block * 8 * step_rows + col, 8, stride=step_rows), :] for block in range(ROWS // 8)
        ]
        tables.append(jnp.concatenate(split3(jnp.concatenate(blocks, 0)), 0))
    table = jnp.concatenate(tables, 1)

    row16 = lax.broadcasted_iota(jnp.int32, (16, LANES), 0)
    one = jnp.ones((16, LANES), jnp.bfloat16)
    zero_one = jnp.zeros((16, LANES), jnp.bfloat16)
    copies = []
    for start in range(0, tiles, GROUP):
        rights = []
        for tile in range(start, start + GROUP):
            gap = (place_ref[pl.ds(tile, 16, stride=0), :] - row16).astype(jnp.int16)
            rights.append(
                jnp.concatenate([jnp.where(gap == jnp.int16(at), one, zero_one) for at in range(0, cams, 16)], 0)
            )
        found = dot_nn(table, jnp.concatenate(rights, 1))
        found = found[0:ROWS] + found[ROWS : 2 * ROWS] + found[2 * ROWS : 3 * ROWS]
        for at in range(GROUP):
            tile = start + at
            here = slice(tile * LANES, (tile + 1) * LANES)
            block = [found[8 * pos : 8 * pos + 8, at * LANES : (at + 1) * LANES] for pos in range(6)]
            red = red_ref[:, here]
            last = last_ref[pl.ds(tile, 8, stride=0), :]
            whole = jnp.where(row < 4, block[4], pltpu.roll(block[4], 4, 0))
            value = block[0] * red + block[5] * last + whole * pltpu.roll(red, 4, 0)
            for gap in range(1, 4):
                value = value + block[gap] * pltpu.roll(red, 8 - gap, 0)
                value = value + pltpu.roll(block[gap] * red, gap, 0)
            out_ref[0:8, here] = value
            edge = jnp.sum(block[5] * red, axis=0, keepdims=True)
            out_ref[8:9, here] = edge + (block[4] * last)[4:5]
        if (start // GROUP) % 2 == 1:
            span = pl.ds((start - GROUP) * LANES, 2 * GROUP * LANES)
            copy = pltpu.make_async_copy(out_ref.at[:, span], out_hbm.at[:, span], sems.at[len(copies)])
            copy.start()
            copies.append(copy)

    want = lax.broadcasted_iota(jnp.int32, (LANES, half), 0) + lax.axis_index(AXES) * owned
    first = jnp.where(slot_ref[pl.ds(grp, 1), :] == want, 1.0, 0.0).astype(jnp.bfloat16)
    second = jnp.where(slot_ref[pl.ds(1 - grp, 1), :] == want, 1.0, 0.0).astype(jnp.bfloat16)
    own = dot_nt(table, jnp.concatenate([first, second], 1))
    own = own[0:ROWS] + own[ROWS : 2 * ROWS] + own[2 * ROWS : 3 * ROWS]
    own_ref[81:LANES, :] = jnp.zeros((LANES - 81, LANES), jnp.float32)
    for row_at in range(9):
        for col_at in range(9):
            at = row_of(row_at, col_at)
            own_ref[row_at * 9 + col_at : row_at * 9 + col_at + 1, :] = own[at : at + 1]
    inv_ref[...] = jnp.transpose(own_ref[...])[0:owned, 0:81]
    for copy in copies:
        copy.wait()


def flips(count, mask):
    return [(at, at ^ mask) for at in range(count)]


def shards(cam_jac, pt_jac, resid, obs_point, obs_camera, camera_slot, *, npts, ngrp):
    count = npts * ngrp
    cams = camera_slot.shape[0]
    half = cams // 2
    owned = cams // count
    size = obs_point.shape[0]
    tiles = size // LANES
    vmem = pl.BlockSpec(memory_space=pltpu.VMEM)
    hbm = pl.BlockSpec(memory_space=pl.ANY)

    def near(value):
        return pltpu.with_memory_space_constraint(value, pltpu.VMEM)

    mine, theirs, red, last, place = pl.pallas_call(
        terms_kernel,
        in_specs=[vmem] * 4 + [hbm],
        out_specs=[vmem] * 5,
        out_shape=[
            pltpu.VMEM((ROWS, half), jnp.float32),
            pltpu.VMEM((ROWS, half), jnp.float32),
            pltpu.VMEM((8, size), jnp.float32),
            pltpu.VMEM((tiles, LANES), jnp.float32),
            pltpu.VMEM((tiles, LANES), jnp.int32),
        ],
        scratch_shapes=[
            pltpu.VMEM(cam_jac.shape, jnp.float32),
            pltpu.VMEM((8 * tiles, LANES), jnp.float32),
            pltpu.VMEM((16 * tiles, LANES), jnp.float32),
            pltpu.VMEM((5 * tiles, LANES), jnp.float32),
            pltpu.VMEM((tiles, LANES), jnp.float32),
            pltpu.SemaphoreType.DMA,
        ],
        name="terms",
    )(pt_jac, resid, obs_point.reshape(tiles, LANES), obs_camera.reshape(tiles, LANES), cam_jac)

    total = mine + lax.ppermute(theirs, AXES, flips(count, 1))
    bit = ngrp
    while bit < count:
        masks = (bit, 2 * bit, 3 * bit) if 2 * bit < count else (bit,)
        got = [lax.ppermute(total, AXES, flips(count, mask)) for mask in masks]
        for value in got:
            total = total + value
        bit *= 4
    theirs = lax.ppermute(total, AXES, flips(count, 1))

    inverse, precond = pl.pallas_call(
        apply_kernel,
        in_specs=[vmem] * 6,
        out_specs=[vmem, hbm],
        out_shape=[
            jax.ShapeDtypeStruct((owned, 81), jnp.float32),
            jax.ShapeDtypeStruct((9, size), jnp.float32),
        ],
        scratch_shapes=[
            pltpu.VMEM((ROWS * max(8, cams // LANES), LANES), jnp.float32),
            pltpu.VMEM((3 * ROWS, cams), jnp.bfloat16),
            pltpu.VMEM((LANES, LANES), jnp.float32),
            pltpu.VMEM((9, size), jnp.float32),
            pltpu.SemaphoreType.DMA((tiles // (2 * GROUP),)),
        ],
        name="apply",
    )(near(total), near(theirs), near(place), near(red), near(last), camera_slot.reshape(2, half))
    return (inverse.T, precond)


def solution(mesh):
    spread = P(None, AXES)
    in_specs = (spread, spread, spread, P(AXES), P(AXES), P())
    body = functools.partial(shards, npts=mesh.shape["pts"], ngrp=mesh.shape["grp"])
    return jax.shard_map(body, mesh=mesh, in_specs=in_specs, out_specs=(spread, spread), check_vma=False)
```

```python
import functools

import jax
import jax.numpy as jnp
from jax import lax
from jax.experimental import pallas as pl
from jax.experimental.pallas import tpu as pltpu
from jax.sharding import PartitionSpec as P

AXES = ("pts", "grp")
DAMP = 1.0
LANES = 128
ROWS = 48
GROUP = 8
SCATTER = 8


def split3(value):
    high = value.astype(jnp.bfloat16)
    rest = value - high.astype(jnp.float32)
    mid = rest.astype(jnp.bfloat16)
    low = (rest - mid.astype(jnp.float32)).astype(jnp.bfloat16)
    return high, mid, low


def dot_nn(left, right):
    return lax.dot_general(left, right, (((1,), (0,)), ((), ())), preferred_element_type=jnp.float32)


def dot_nt(left, right):
    return lax.dot_general(left, right, (((1,), (1,)), ((), ())), preferred_element_type=jnp.float32)


def row_of(row_at, col_at):
    if row_at == 8 and col_at == 8:
        return 36
    if row_at == 8:
        return 40 + col_at
    if col_at == 8:
        return 40 + row_at
    gap = (col_at - row_at) % 8
    if gap > 4 or (gap == 4 and row_at >= 4):
        return 8 * ((row_at - col_at) % 8) + col_at
    return 8 * gap + row_at


def side_of(device):
    for shift in (8, 4, 2, 1):
        device = device ^ (device >> shift)
    return device & 1


def other_half(named, side, half):
    swapped = jnp.where(named < half, named + half, named - half)
    return jnp.where(side == 0, named, swapped)


def terms_kernel(
    pt_ref, res_ref, point_ref, named_ref, cam_hbm,
    mine_ref, theirs_ref, red_ref, last_ref, place_ref,
    cam_ref, dense_ref, total_ref, keep_ref, where_ref, sem,
):
    tiles = point_ref.shape[0]
    half = mine_ref.shape[1]
    cams = 2 * half
    load = pltpu.make_async_copy(cam_hbm, cam_ref, sem)
    load.start()
    row = lax.broadcasted_iota(jnp.int32, (8, LANES), 0)
    where_ref[...] = (point_ref[...] - point_ref[0:1, 0:1]).astype(jnp.float32)
    place_ref[...] = other_half(named_ref[...], side_of(lax.axis_index(AXES)), half)
    one = jnp.ones((LANES, LANES), jnp.bfloat16)
    zero_one = jnp.zeros((LANES, LANES), jnp.bfloat16)

    camera_columns = []
    for start in range(0, tiles, GROUP):
        points = where_ref[start : start + GROUP, :]
        both_ids = jnp.concatenate([points, place_ref[start : start + GROUP, :].astype(jnp.float32)], 0)
        columns = jnp.transpose(both_ids).astype(jnp.int32).astype(jnp.int16)
        camera_columns.append(columns)
        points = points.astype(jnp.int32)
        for at in range(GROUP):
            tile = start + at
            here = slice(tile * LANES, (tile + 1) * LANES)
            value = jnp.concatenate([pt_ref[:, here], res_ref[:, here]], 0)
            shift1 = pltpu.roll(value, 7, 0)
            shift2 = pltpu.roll(value, 6, 0)
            error = jnp.where(row < 3, value[6:7], value[7:8])

            def both(prod):
                return prod + pltpu.roll(prod, 5, 0)

            upper = jnp.where(
                row < 3,
                both(value * value),
                jnp.where(
                    row < 5,
                    pltpu.roll(both(value * shift1), 3, 0),
                    pltpu.roll(both(value * shift2), 5, 0),
                ),
            )
            lower = both(value * error)
            left = jnp.concatenate(split3(jnp.concatenate([upper, lower], 0)), 0)
            line = jnp.broadcast_to(points[at : at + 1], (16, LANES)).astype(jnp.int16)
            same = jnp.where(
                jnp.broadcast_to(columns[:, at : at + 1], (LANES, LANES)) == jnp.concatenate([line] * 8, 0),
                one,
                zero_one,
            )
            found = dot_nn(left, same)
            found = found[0:16] + found[16:32] + found[32:48]
            total_ref[pl.ds(tile, 8, stride=tiles), :] = found[0:8]
            total_ref[pl.ds(8 * tiles + tile, 8, stride=tiles), :] = found[8:16]
            dense_ref[pl.ds(tile, 8, stride=tiles), :] = value

    places = where_ref[...]
    turned = jnp.transpose(places)
    tile_at = lax.broadcasted_iota(jnp.int32, (tiles, tiles), 0)
    other = lax.broadcasted_iota(jnp.int32, (tiles, tiles), 1)
    before = jnp.where((other < tile_at) & (turned[LANES - 1 : LANES, :] == places[:, 0:1]), 1.0, 0.0)
    after = jnp.where((other > tile_at) & (turned[0:1, :] == places[:, LANES - 1 : LANES]), 1.0, 0.0)
    lane_at = lax.broadcasted_iota(jnp.int32, (tiles, LANES), 1)
    heads = jnp.zeros((tiles, LANES), jnp.float32)
    tails = jnp.zeros((tiles, LANES), jnp.float32)
    for pos in (0, 1, 2, 3, 4, 5, 8, 9, 10):
        found = total_ref[pos * tiles : (pos + 1) * tiles, :]
        heads = jnp.where(lane_at == pos, found[:, 0:1], heads)
        tails = jnp.where(lane_at == pos, found[:, LANES - 1 : LANES], tails)

    def carried(matrix, column):
        parts = [dot_nn(matrix.astype(jnp.bfloat16), part) for part in split3(column)]
        return parts[0] + parts[1] + parts[2]

    from_before = carried(before, tails)
    from_after = carried(after, heads)

    for start in range(0, tiles, 8):
        place = places[start : start + 8]
        is_head = place == place[:, 0:1]
        is_tail = place == place[:, LANES - 1 : LANES]
        add_before = from_before[start : start + 8]
        add_after = from_after[start : start + 8]

        def total(pos):
            value = total_ref[pos * tiles + start : pos * tiles + start + 8, :]
            value = value + jnp.where(is_head, add_before[:, pos : pos + 1], 0.0)
            return value + jnp.where(is_tail, add_after[:, pos : pos + 1], 0.0)

        v00, v11, v22 = [total(pos) + DAMP for pos in (0, 1, 2)]
        v01, v12, v02 = [total(pos) for pos in (3, 4, 5)]
        bees = [total(pos) for pos in (8, 9, 10)]
        dense = [dense_ref[pos * tiles + start : pos * tiles + start + 8, :] for pos in range(8)]
        c00 = v11 * v22 - v12 * v12
        c01 = v02 * v12 - v01 * v22
        c02 = v01 * v12 - v02 * v11
        c11 = v00 * v22 - v02 * v02
        c12 = v01 * v02 - v00 * v12
        c22 = v00 * v11 - v01 * v01
        scale = 1.0 / (v00 * c00 + v01 * c01 + v02 * c02)
        vinv = [[c00 * scale, c01 * scale, c02 * scale]]
        vinv.append([vinv[0][1], c11 * scale, c12 * scale])
        vinv.append([vinv[0][2], vinv[1][2], c22 * scale])

        def times(vec):
            return [vinv[at][0] * vec[0] + vinv[at][1] * vec[1] + vinv[at][2] * vec[2] for at in range(3)]

        def inner(left, right):
            return left[0] * right[0] + left[1] * right[1] + left[2] * right[2]

        top, low = dense[0:3], dense[3:6]
        use_top, use_low, weight = times(top), times(low), times(bees)
        results = (
            1.0 - inner(top, use_top),
            -inner(top, use_low),
            1.0 - inner(low, use_low),
            dense[6] - inner(top, weight),
            dense[7] - inner(low, weight),
        )
        for pos, value in enumerate(results):
            keep_ref[pos * tiles + start : pos * tiles + start + 8, :] = value

    load.wait()
    lane16 = lax.broadcasted_iota(jnp.int32, (16, LANES), 1)
    names = [(lane16 + at * LANES).astype(jnp.int16) for at in range(cams // LANES)]
    one = jnp.ones((16, LANES), jnp.bfloat16)
    zero_one = jnp.zeros((16, LANES), jnp.bfloat16)
    acc = jnp.zeros((3 * ROWS, cams), jnp.float32)
    for start in range(0, tiles, SCATTER):
        lefts = []
        rights = []
        for tile in range(start, start + SCATTER):
            here = slice(tile * LANES, (tile + 1) * LANES)

            def spread(ref, at):
                return ref[pl.ds(at, 8, stride=0), :]

            k00, k01, k11, s0, s1 = [spread(keep_ref, pos * tiles + tile) for pos in range(5)]
            zero, one_row = cam_ref[0:8, here], cam_ref[9:17, here]
            zero8 = jnp.broadcast_to(cam_ref[8:9, here], (8, LANES))
            one8 = jnp.broadcast_to(cam_ref[17:18, here], (8, LANES))
            m0 = k00 * zero + k01 * one_row
            m1 = k01 * zero + k11 * one_row
            corner = zero8 * (k00 * zero8 + k01 * one8) + one8 * (k01 * zero8 + k11 * one8)
            pieces = [zero * m0 + one_row * m1]
            for gap in range(1, 5):
                pieces.append(zero * pltpu.roll(m0, 8 - gap, 0) + one_row * pltpu.roll(m1, 8 - gap, 0))
            pieces[4] = jnp.where(row == 4, corner, pieces[4])
            pieces.append(zero8 * m0 + one8 * m1)
            lefts.append(jnp.concatenate(split3(jnp.concatenate(pieces, 0)), 0))
            red_ref[:, here] = zero * s0 + one_row * s1
            last_ref[tile : tile + 1, :] = (zero8 * s0 + one8 * s1)[0:1]
            source = camera_columns[tile // GROUP]
            lane = GROUP + tile % GROUP
            for at in range(0, LANES, 16):
                column = jnp.broadcast_to(source[at : at + 16, lane : lane + 1], (16, LANES))
                rights.append(jnp.concatenate([jnp.where(column == name, one, zero_one) for name in names], 1))
        acc = acc + dot_nn(jnp.concatenate(lefts, 1), jnp.concatenate(rights, 0))
    done = acc[0:ROWS] + acc[ROWS : 2 * ROWS] + acc[2 * ROWS : 3 * ROWS]
    mine_ref[...] = done[:, 0:half]
    theirs_ref[...] = done[:, half:cams]


def inverse_of(entry):
    entry = dict(entry)
    root = {}
    factor = {}
    for col_at in range(9):
        root[col_at] = lax.rsqrt(entry[col_at, col_at])
        for row_at in range(col_at + 1, 9):
            factor[row_at, col_at] = entry[row_at, col_at] * root[col_at]
        for row_at in range(col_at + 1, 9):
            for inner in range(col_at + 1, row_at + 1):
                entry[row_at, inner] = entry[row_at, inner] - factor[row_at, col_at] * factor[inner, col_at]
    solved = {}
    for col_at in range(9):
        solved[col_at, col_at] = root[col_at]
        for row_at in range(col_at + 1, 9):
            value = factor[row_at, col_at] * solved[col_at, col_at]
            for inner in range(col_at + 1, row_at):
                value = value + factor[row_at, inner] * solved[inner, col_at]
            solved[row_at, col_at] = -value * root[row_at]
    result = {}
    for row_at in range(9):
        for col_at in range(row_at + 1):
            value = solved[row_at, row_at] * solved[row_at, col_at]
            for inner in range(row_at + 1, 9):
                value = value + solved[inner, row_at] * solved[inner, col_at]
            result[row_at, col_at] = value
    return result


def apply_kernel(
    mine_ref, theirs_ref, place_ref, red_ref, last_ref, slot_ref,
    inv_hbm, out_hbm,
    entry_ref, own_ref, turned_ref, out_ref, sems, own_sem,
):
    tiles = place_ref.shape[0]
    half = mine_ref.shape[1]
    cams = 2 * half
    owned = inv_hbm.shape[0]
    cols = cams // LANES
    side = side_of(lax.axis_index(AXES))
    row = lax.broadcasted_iota(jnp.int32, (8, LANES), 0)
    step_rows = entry_ref.shape[0] // ROWS
    for block in range(ROWS // 8):
        for col in range(cols):
            source = mine_ref if col < cols // 2 else theirs_ref
            at = (col % (cols // 2)) * LANES
            entry_ref[pl.ds(block * 8 * step_rows + col, 8, stride=step_rows), :] = source[
                block * 8 : block * 8 + 8, at : at + LANES
            ]

    def entry_at(row_at, col_at):
        at = row_of(row_at, col_at) * step_rows
        return entry_ref[at : at + cols, :]

    entry = {(r, c): entry_at(r, c) for r in range(9) for c in range(r + 1)}
    for at in range(9):
        entry[at, at] = entry[at, at] + DAMP
    result = inverse_of(entry)
    spare = jnp.zeros((cols, LANES), jnp.float32)
    for at in (37, 38, 39):
        entry_ref[at * step_rows : at * step_rows + cols, :] = spare
    for (row_at, col_at), value in result.items():
        at = row_of(row_at, col_at) * step_rows
        entry_ref[at : at + cols, :] = value
    tables = []
    for col in range(cols):
        blocks = [
            entry_ref[pl.ds(block * 8 * step_rows + col, 8, stride=step_rows), :] for block in range(ROWS // 8)
        ]
        tables.append(jnp.concatenate(split3(jnp.concatenate(blocks, 0)), 0))
    table = jnp.concatenate(tables, 1)

    row16 = lax.broadcasted_iota(jnp.int32, (16, LANES), 0)
    one = jnp.ones((16, LANES), jnp.bfloat16)
    zero_one = jnp.zeros((16, LANES), jnp.bfloat16)
    want = lax.broadcasted_iota(jnp.int32, (LANES, half), 0) + lax.axis_index(AXES) * owned
    first = jnp.where(slot_ref[pl.ds(side, 1), :] == want, 1.0, 0.0).astype(jnp.bfloat16)
    second = jnp.where(slot_ref[pl.ds(1 - side, 1), :] == want, 1.0, 0.0).astype(jnp.bfloat16)
    own = dot_nt(table, jnp.concatenate([first, second], 1))
    own = own[0:ROWS] + own[ROWS : 2 * ROWS] + own[2 * ROWS : 3 * ROWS]
    own_ref[81:LANES, :] = jnp.zeros((LANES - 81, LANES), jnp.float32)
    for row_at in range(9):
        for col_at in range(9):
            at = row_of(row_at, col_at)
            own_ref[row_at * 9 + col_at : row_at * 9 + col_at + 1, :] = own[at : at + 1]
    turned_ref[...] = jnp.transpose(own_ref[...])[0:owned, 0:81]
    own_copy = pltpu.make_async_copy(turned_ref, inv_hbm, own_sem)
    own_copy.start()
    copies = []
    for start in range(0, tiles, GROUP):
        rights = []
        for tile in range(start, start + GROUP):
            gap = (place_ref[pl.ds(tile, 16, stride=0), :] - row16).astype(jnp.int16)
            rights.append(
                jnp.concatenate([jnp.where(gap == jnp.int16(at), one, zero_one) for at in range(0, cams, 16)], 0)
            )
        found = dot_nn(table, jnp.concatenate(rights, 1))
        found = found[0:ROWS] + found[ROWS : 2 * ROWS] + found[2 * ROWS : 3 * ROWS]
        for at in range(GROUP):
            tile = start + at
            here = slice(tile * LANES, (tile + 1) * LANES)
            block = [found[8 * pos : 8 * pos + 8, at * LANES : (at + 1) * LANES] for pos in range(6)]
            red = red_ref[:, here]
            last = last_ref[pl.ds(tile, 8, stride=0), :]
            whole = jnp.where(row < 4, block[4], pltpu.roll(block[4], 4, 0))
            value = block[0] * red + block[5] * last + whole * pltpu.roll(red, 4, 0)
            for gap in range(1, 4):
                value = value + block[gap] * pltpu.roll(red, 8 - gap, 0)
                value = value + pltpu.roll(block[gap] * red, gap, 0)
            out_ref[0:8, here] = value
            edge = jnp.sum(block[5] * red, axis=0, keepdims=True)
            out_ref[8:9, here] = edge + (block[4] * last)[4:5]
        span = pl.ds(start * LANES, GROUP * LANES)
        copy = pltpu.make_async_copy(out_ref.at[:, span], out_hbm.at[:, span], sems.at[start // GROUP])
        copy.start()
        copies.append(copy)

    own_copy.wait()
    for copy in copies:
        copy.wait()


def partners(count, mask):
    return [(at, at ^ mask) for at in range(count)]


def exchange_steps(npts):
    bits = [1 << at for at in range(npts.bit_length() - 1)]
    if len(bits) < 3:
        return [(bit,) for bit in bits]
    return [(bit,) for bit in bits[2:-1]] + [(bits[0], bits[1], bits[0] + bits[1]), (bits[-1],)]


def shards(cam_jac, pt_jac, resid, obs_point, obs_camera, camera_slot, *, npts, ngrp):
    count = npts * ngrp
    cams = camera_slot.shape[0]
    half = cams // 2
    owned = cams // count
    size = obs_point.shape[0]
    tiles = size // LANES
    vmem = pl.BlockSpec(memory_space=pltpu.VMEM)
    hbm = pl.BlockSpec(memory_space=pl.ANY)

    def near(value):
        return pltpu.with_memory_space_constraint(value, pltpu.VMEM)

    mine, theirs, red, last, place = pl.pallas_call(
        terms_kernel,
        in_specs=[vmem] * 4 + [hbm],
        out_specs=[vmem] * 5,
        out_shape=[
            pltpu.VMEM((ROWS, half), jnp.float32),
            pltpu.VMEM((ROWS, half), jnp.float32),
            pltpu.VMEM((8, size), jnp.float32),
            pltpu.VMEM((tiles, LANES), jnp.float32),
            pltpu.VMEM((tiles, LANES), jnp.int32),
        ],
        scratch_shapes=[
            pltpu.VMEM(cam_jac.shape, jnp.float32),
            pltpu.VMEM((8 * tiles, LANES), jnp.float32),
            pltpu.VMEM((16 * tiles, LANES), jnp.float32),
            pltpu.VMEM((5 * tiles, LANES), jnp.float32),
            pltpu.VMEM((tiles, LANES), jnp.float32),
            pltpu.SemaphoreType.DMA,
        ],
        name="terms",
    )(pt_jac, resid, obs_point.reshape(tiles, LANES), obs_camera.reshape(tiles, LANES), cam_jac)

    total = mine + lax.ppermute(theirs, AXES, partners(count, 1))
    for masks in exchange_steps(npts):
        got = [lax.ppermute(total, AXES, partners(count, mask * ngrp + mask.bit_count() % 2)) for mask in masks]
        for value in got:
            total = total + value
    theirs = lax.ppermute(total, AXES, partners(count, 1))

    inverse, precond = pl.pallas_call(
        apply_kernel,
        in_specs=[vmem] * 6,
        out_specs=[hbm, hbm],
        out_shape=[
            jax.ShapeDtypeStruct((owned, 81), jnp.float32),
            jax.ShapeDtypeStruct((9, size), jnp.float32),
        ],
        scratch_shapes=[
            pltpu.VMEM((ROWS * max(8, cams // LANES), LANES), jnp.float32),
            pltpu.VMEM((LANES, LANES), jnp.float32),
            pltpu.VMEM((owned, 81), jnp.float32),
            pltpu.VMEM((9, size), jnp.float32),
            pltpu.SemaphoreType.DMA((tiles // GROUP,)),
            pltpu.SemaphoreType.DMA,
        ],
        name="apply",
    )(near(total), near(theirs), near(place), near(red), near(last), near(camera_slot.reshape(2, half)))
    return (inverse.T, precond)


def solution(mesh):
    spread = P(None, AXES)
    in_specs = (spread, spread, spread, P(AXES), P(AXES), P())
    body = functools.partial(shards, npts=mesh.shape["pts"], ngrp=mesh.shape["grp"])
    return jax.shard_map(body, mesh=mesh, in_specs=in_specs, out_specs=(spread, spread), check_vma=False)
```

```python
import functools

import jax
import jax.numpy as jnp
from jax import lax
from jax.experimental import pallas as pl
from jax.experimental.pallas import tpu as pltpu
from jax.sharding import PartitionSpec as P

AXES = ("pts", "grp")
DAMP = 1.0
LANES = 128
ROWS = 48
GROUP = 8
SCATTER = 8


def split3(value):
    high = value.astype(jnp.bfloat16)
    rest = value - high.astype(jnp.float32)
    mid = rest.astype(jnp.bfloat16)
    low = (rest - mid.astype(jnp.float32)).astype(jnp.bfloat16)
    return high, mid, low


def dot_nn(left, right):
    return lax.dot_general(left, right, (((1,), (0,)), ((), ())), preferred_element_type=jnp.float32)


def dot_nt(left, right):
    return lax.dot_general(left, right, (((1,), (1,)), ((), ())), preferred_element_type=jnp.float32)


def row_of(row_at, col_at):
    if row_at == 8 and col_at == 8:
        return 36
    if row_at == 8:
        return 40 + col_at
    if col_at == 8:
        return 40 + row_at
    gap = (col_at - row_at) % 8
    if gap > 4 or (gap == 4 and row_at >= 4):
        return 8 * ((row_at - col_at) % 8) + col_at
    return 8 * gap + row_at


def side_of(device):
    for shift in (8, 4, 2, 1):
        device = device ^ (device >> shift)
    return device & 1


def other_half(named, side, half):
    swapped = jnp.where(named < half, named + half, named - half)
    return jnp.where(side == 0, named, swapped)


def terms_kernel(
    pt_ref, res_ref, point_ref, named_ref, cam_hbm,
    mine_ref, theirs_ref, red_ref, last_ref, place_ref,
    cam_ref, dense_ref, total_ref, keep_ref, where_ref, sem,
):
    tiles = point_ref.shape[0]
    half = mine_ref.shape[1]
    cams = 2 * half
    load = pltpu.make_async_copy(cam_hbm, cam_ref, sem)
    load.start()
    row = lax.broadcasted_iota(jnp.int32, (8, LANES), 0)
    where_ref[...] = (point_ref[...] - point_ref[0:1, 0:1]).astype(jnp.float32)
    place_ref[...] = other_half(named_ref[...], side_of(lax.axis_index(AXES)), half)
    one = jnp.ones((LANES, LANES), jnp.bfloat16)
    zero_one = jnp.zeros((LANES, LANES), jnp.bfloat16)
    lane = lax.broadcasted_iota(jnp.int32, (16, LANES), 1)
    all_columns = []
    all_points = []
    for start in range(0, tiles, GROUP):
        points = where_ref[start : start + GROUP, :]
        both_ids = jnp.concatenate([points, place_ref[start : start + GROUP, :].astype(jnp.float32)], 0)
        all_points.append(points.astype(jnp.int32))
        all_columns.append(jnp.transpose(both_ids).astype(jnp.int32).astype(jnp.int16))

    places = where_ref[...]
    turned = jnp.concatenate([jnp.transpose(places), jnp.full((LANES, LANES - tiles), -1.0, jnp.float32)], 1)
    tile_at = lax.broadcasted_iota(jnp.int32, (tiles, LANES), 1)
    other = lax.broadcasted_iota(jnp.int32, (tiles, LANES), 0)
    before = (other < tile_at) & (turned[0:1, :] == places[:, LANES - 1 : LANES])
    after = (other > tile_at) & (turned[LANES - 1 : LANES, :] == places[:, 0:1])
    before = jnp.where(before, 1.0, 0.0).astype(jnp.bfloat16)
    after = jnp.where(after, 1.0, 0.0).astype(jnp.bfloat16)

    head_rows = jnp.where(places == places[:, 0:1], 1.0, 0.0)
    tail_rows = jnp.where(places == places[:, LANES - 1 : LANES], 1.0, 0.0)
    heads = jnp.zeros((16, LANES), jnp.float32)
    tails = jnp.zeros((16, LANES), jnp.float32)
    lefts = []
    wholes = []
    for tile in range(tiles):
        here = slice(tile * LANES, (tile + 1) * LANES)
        value = jnp.concatenate([pt_ref[:, here], res_ref[:, here]], 0)
        shift1 = pltpu.roll(value, 7, 0)
        shift2 = pltpu.roll(value, 6, 0)
        error = jnp.where(row < 3, value[6:7], value[7:8])

        def both(prod):
            return prod + pltpu.roll(prod, 5, 0)

        upper = jnp.where(
            row < 3,
            both(value * value),
            jnp.where(
                row < 5,
                pltpu.roll(both(value * shift1), 3, 0),
                pltpu.roll(both(value * shift2), 5, 0),
            ),
        )
        whole = jnp.concatenate([upper, both(value * error)], 0)
        lefts.append(jnp.concatenate(split3(whole), 0))
        wholes.append(whole)
        dense_ref[pl.ds(tile, 8, stride=tiles), :] = value

    for tile in range(tiles // 2):
        columns = all_columns[tile // GROUP]
        at = tile % GROUP
        line = jnp.broadcast_to(all_points[tile // GROUP][at : at + 1], (16, LANES)).astype(jnp.int16)
        same = jnp.where(
            jnp.broadcast_to(columns[:, at : at + 1], (LANES, LANES)) == jnp.concatenate([line] * 8, 0),
            one,
            zero_one,
        )
        found = dot_nn(lefts[tile], same)
        found = found[0:16] + found[16:32] + found[32:48]
        total_ref[pl.ds(tile, 8, stride=tiles), :] = found[0:8]
        total_ref[pl.ds(8 * tiles + tile, 8, stride=tiles), :] = found[8:16]

    for tile in range(tiles):
        whole = wholes[tile]
        heads = jnp.where(lane == tile, jnp.sum(whole * head_rows[tile : tile + 1], axis=1, keepdims=True), heads)
        tails = jnp.where(lane == tile, jnp.sum(whole * tail_rows[tile : tile + 1], axis=1, keepdims=True), tails)

    def carried(rows, matrix):
        found = dot_nn(jnp.concatenate(split3(rows), 0)[:, 0:tiles], matrix)
        return found[0:16] + found[16:32] + found[32:48]

    carry = jnp.transpose(jnp.concatenate([carried(tails, before), carried(heads, after)], 0))
    from_before = carry[:, 0:16]
    from_after = carry[:, 16:32]

    for tile in range(tiles // 2, tiles):
        columns = all_columns[tile // GROUP]
        at = tile % GROUP
        line = jnp.broadcast_to(all_points[tile // GROUP][at : at + 1], (16, LANES)).astype(jnp.int16)
        same = jnp.where(
            jnp.broadcast_to(columns[:, at : at + 1], (LANES, LANES)) == jnp.concatenate([line] * 8, 0),
            one,
            zero_one,
        )
        found = dot_nn(lefts[tile], same)
        found = found[0:16] + found[16:32] + found[32:48]
        total_ref[pl.ds(tile, 8, stride=tiles), :] = found[0:8]
        total_ref[pl.ds(8 * tiles + tile, 8, stride=tiles), :] = found[8:16]

    for start in range(0, tiles, 8):
        is_head = head_rows[start : start + 8]
        is_tail = tail_rows[start : start + 8]
        add_before = from_before[start : start + 8]
        add_after = from_after[start : start + 8]

        def total(pos):
            value = total_ref[pos * tiles + start : pos * tiles + start + 8, :]
            return value + is_head * add_before[:, pos : pos + 1] + is_tail * add_after[:, pos : pos + 1]

        v00, v11, v22 = [total(pos) + DAMP for pos in (0, 1, 2)]
        v01, v12, v02 = [total(pos) for pos in (3, 4, 5)]
        bees = [total(pos) for pos in (8, 9, 10)]
        dense = [dense_ref[pos * tiles + start : pos * tiles + start + 8, :] for pos in range(8)]
        c00 = v11 * v22 - v12 * v12
        c01 = v02 * v12 - v01 * v22
        c02 = v01 * v12 - v02 * v11
        c11 = v00 * v22 - v02 * v02
        c12 = v01 * v02 - v00 * v12
        c22 = v00 * v11 - v01 * v01
        scale = 1.0 / (v00 * c00 + v01 * c01 + v02 * c02)
        vinv = [[c00 * scale, c01 * scale, c02 * scale]]
        vinv.append([vinv[0][1], c11 * scale, c12 * scale])
        vinv.append([vinv[0][2], vinv[1][2], c22 * scale])

        def times(vec):
            return [vinv[at][0] * vec[0] + vinv[at][1] * vec[1] + vinv[at][2] * vec[2] for at in range(3)]

        def inner(left, right):
            return left[0] * right[0] + left[1] * right[1] + left[2] * right[2]

        top, low = dense[0:3], dense[3:6]
        use_top, use_low, weight = times(top), times(low), times(bees)
        results = (
            1.0 - inner(top, use_top),
            -inner(top, use_low),
            1.0 - inner(low, use_low),
            dense[6] - inner(top, weight),
            dense[7] - inner(low, weight),
        )
        for pos, value in enumerate(results):
            keep_ref[pos * tiles + start : pos * tiles + start + 8, :] = value

    load.wait()
    lane16 = lax.broadcasted_iota(jnp.int32, (16, LANES), 1)
    names = [(lane16 + at * LANES).astype(jnp.int16) for at in range(cams // LANES)]
    one = jnp.ones((16, LANES), jnp.bfloat16)
    zero_one = jnp.zeros((16, LANES), jnp.bfloat16)
    acc = jnp.zeros((3 * ROWS, cams), jnp.float32)
    for start in range(0, tiles, SCATTER):
        lefts = []
        rights = []
        for tile in range(start, start + SCATTER):
            here = slice(tile * LANES, (tile + 1) * LANES)

            def spread(ref, at):
                return ref[pl.ds(at, 8, stride=0), :]

            k00, k01, k11, s0, s1 = [spread(keep_ref, pos * tiles + tile) for pos in range(5)]
            zero, one_row = cam_ref[0:8, here], cam_ref[9:17, here]
            zero8 = jnp.broadcast_to(cam_ref[8:9, here], (8, LANES))
            one8 = jnp.broadcast_to(cam_ref[17:18, here], (8, LANES))
            m0 = k00 * zero + k01 * one_row
            m1 = k01 * zero + k11 * one_row
            corner = zero8 * (k00 * zero8 + k01 * one8) + one8 * (k01 * zero8 + k11 * one8)
            pieces = [zero * m0 + one_row * m1]
            for gap in range(1, 5):
                pieces.append(zero * pltpu.roll(m0, 8 - gap, 0) + one_row * pltpu.roll(m1, 8 - gap, 0))
            pieces[4] = jnp.where(row == 4, corner, pieces[4])
            pieces.append(zero8 * m0 + one8 * m1)
            lefts.append(jnp.concatenate(split3(jnp.concatenate(pieces, 0)), 0))
            red_ref[:, here] = zero * s0 + one_row * s1
            last_ref[tile : tile + 1, :] = (zero8 * s0 + one8 * s1)[0:1]
            source = all_columns[tile // GROUP]
            column_at = GROUP + tile % GROUP
            for at in range(0, LANES, 16):
                column = jnp.broadcast_to(source[at : at + 16, column_at : column_at + 1], (16, LANES))
                rights.append(jnp.concatenate([jnp.where(column == name, one, zero_one) for name in names], 1))
        acc = acc + dot_nn(jnp.concatenate(lefts, 1), jnp.concatenate(rights, 0))
    done = acc[0:ROWS] + acc[ROWS : 2 * ROWS] + acc[2 * ROWS : 3 * ROWS]
    mine_ref[...] = done[:, 0:half]
    theirs_ref[...] = done[:, half:cams]


def inverse_of(entry):
    entry = dict(entry)
    root = {}
    factor = {}
    for col_at in range(9):
        root[col_at] = lax.rsqrt(entry[col_at, col_at])
        for row_at in range(col_at + 1, 9):
            factor[row_at, col_at] = entry[row_at, col_at] * root[col_at]
        for row_at in range(col_at + 1, 9):
            for inner in range(col_at + 1, row_at + 1):
                entry[row_at, inner] = entry[row_at, inner] - factor[row_at, col_at] * factor[inner, col_at]
    solved = {}
    for col_at in range(9):
        solved[col_at, col_at] = root[col_at]
        for row_at in range(col_at + 1, 9):
            value = factor[row_at, col_at] * solved[col_at, col_at]
            for inner in range(col_at + 1, row_at):
                value = value + factor[row_at, inner] * solved[inner, col_at]
            solved[row_at, col_at] = -value * root[row_at]
    result = {}
    for row_at in range(9):
        for col_at in range(row_at + 1):
            value = solved[row_at, row_at] * solved[row_at, col_at]
            for inner in range(row_at + 1, 9):
                value = value + solved[inner, row_at] * solved[inner, col_at]
            result[row_at, col_at] = value
    return result


def inverse_table(source_ref, entry_ref):
    half = source_ref.shape[1]
    cols = half // LANES
    step_rows = entry_ref.shape[0] // ROWS
    for block in range(ROWS // 8):
        for col in range(cols):
            entry_ref[pl.ds(block * 8 * step_rows + col, 8, stride=step_rows), :] = source_ref[
                block * 8 : block * 8 + 8, col * LANES : (col + 1) * LANES
            ]

    def entry_at(row_at, col_at):
        at = row_of(row_at, col_at) * step_rows
        return entry_ref[at : at + cols, :]

    entry = {(r, c): entry_at(r, c) for r in range(9) for c in range(r + 1)}
    for at in range(9):
        entry[at, at] = entry[at, at] + DAMP
    result = inverse_of(entry)
    spare = jnp.zeros((cols, LANES), jnp.float32)
    for at in (37, 38, 39):
        entry_ref[at * step_rows : at * step_rows + cols, :] = spare
    for (row_at, col_at), value in result.items():
        at = row_of(row_at, col_at) * step_rows
        entry_ref[at : at + cols, :] = value
    tables = []
    for col in range(cols):
        blocks = [
            entry_ref[pl.ds(block * 8 * step_rows + col, 8, stride=step_rows), :] for block in range(ROWS // 8)
        ]
        tables.append(jnp.concatenate(split3(jnp.concatenate(blocks, 0)), 0))
    return jnp.concatenate(tables, 1)


def add_parts(found):
    return found[0:ROWS] + found[ROWS : 2 * ROWS] + found[2 * ROWS : 3 * ROWS]


def owned_columns(table, slot_ref, at, owned):
    want = lax.broadcasted_iota(jnp.int32, (LANES, slot_ref.shape[1]), 0) + lax.axis_index(AXES) * owned
    pick = jnp.where(slot_ref[pl.ds(at, 1), :] == want, 1.0, 0.0).astype(jnp.bfloat16)
    return add_parts(dot_nt(table, pick))


def applied(table, place_ref, red_ref, last_ref, first, start):
    half = table.shape[1]
    row = lax.broadcasted_iota(jnp.int32, (8, LANES), 0)
    row16 = lax.broadcasted_iota(jnp.int32, (16, LANES), 0) + first
    one = jnp.ones((16, LANES), jnp.bfloat16)
    zero_one = jnp.zeros((16, LANES), jnp.bfloat16)
    rights = []
    for tile in range(start, start + GROUP):
        gap = (place_ref[pl.ds(tile, 16, stride=0), :] - row16).astype(jnp.int16)
        rights.append(
            jnp.concatenate([jnp.where(gap == jnp.int16(at), one, zero_one) for at in range(0, half, 16)], 0)
        )
    found = add_parts(dot_nn(table, jnp.concatenate(rights, 1)))
    results = []
    for at in range(GROUP):
        tile = start + at
        here = slice(tile * LANES, (tile + 1) * LANES)
        block = [found[8 * pos : 8 * pos + 8, at * LANES : (at + 1) * LANES] for pos in range(6)]
        red = red_ref[:, here]
        last = last_ref[pl.ds(tile, 8, stride=0), :]
        whole = jnp.where(row < 4, block[4], pltpu.roll(block[4], 4, 0))
        value = block[0] * red + block[5] * last + whole * pltpu.roll(red, 4, 0)
        for gap in range(1, 4):
            value = value + block[gap] * pltpu.roll(red, 8 - gap, 0)
            value = value + pltpu.roll(block[gap] * red, gap, 0)
        edge = jnp.sum(block[5] * red, axis=0, keepdims=True)
        results.append((tile, here, value, edge + (block[4] * last)[4:5]))
    return results


def first_half_kernel(
    mine_ref, place_ref, red_ref, last_ref, slot_ref,
    own_ref, part_ref, edge_ref,
    entry_ref, *, owned,
):
    table = inverse_table(mine_ref, entry_ref)
    for start in range(0, place_ref.shape[0], GROUP):
        for tile, here, value, edge in applied(table, place_ref, red_ref, last_ref, 0, start):
            part_ref[:, here] = value
            edge_ref[tile : tile + 1, :] = edge
    own_ref[...] = owned_columns(table, slot_ref, side_of(lax.axis_index(AXES)), owned)


def second_half_kernel(
    theirs_ref, place_ref, red_ref, last_ref, slot_ref, own_ref, part_ref, edge_ref,
    inv_hbm, out_hbm,
    entry_ref, square_ref, turned_ref, out_ref, sems, own_sem,
):
    tiles, half = place_ref.shape[0], theirs_ref.shape[1]
    owned = inv_hbm.shape[0]
    table = inverse_table(theirs_ref, entry_ref)
    own = own_ref[...] + owned_columns(table, slot_ref, 1 - side_of(lax.axis_index(AXES)), owned)
    square_ref[81:LANES, :] = jnp.zeros((LANES - 81, LANES), jnp.float32)
    for row_at in range(9):
        for col_at in range(9):
            at = row_of(row_at, col_at)
            square_ref[row_at * 9 + col_at : row_at * 9 + col_at + 1, :] = own[at : at + 1]
    turned_ref[...] = jnp.transpose(square_ref[...])[0:owned, 0:81]
    own_copy = pltpu.make_async_copy(turned_ref, inv_hbm, own_sem)
    own_copy.start()
    copies = []
    for start in range(0, tiles, GROUP):
        for tile, here, value, edge in applied(table, place_ref, red_ref, last_ref, half, start):
            out_ref[0:8, here] = value + part_ref[:, here]
            out_ref[8:9, here] = edge + edge_ref[tile : tile + 1, :]
        span = pl.ds(start * LANES, GROUP * LANES)
        copy = pltpu.make_async_copy(out_ref.at[:, span], out_hbm.at[:, span], sems.at[start // GROUP])
        copy.start()
        copies.append(copy)
    own_copy.wait()
    for copy in copies:
        copy.wait()


def partners(count, ngrp, masks):
    pairs = []
    for at in range(count):
        mask = masks[at.bit_count() % 2]
        pairs.append((at, at ^ (mask * ngrp + mask.bit_count() % 2)))
    return pairs


def exchange_steps(npts):
    bits = [1 << at for at in range(npts.bit_length() - 1)]
    pairs = [(bits[at], bits[at + 1], bits[at] + bits[at + 1]) for at in range(0, len(bits) - 1, 2)]
    turned = pairs[1:] + pairs[:1]
    steps = [list(zip(one, two)) for one, two in zip(pairs, turned)]
    if len(bits) % 2 == 1:
        steps.append([(bits[-1], bits[-1])])
    return steps


def shards(cam_jac, pt_jac, resid, obs_point, obs_camera, camera_slot, *, npts, ngrp):
    count = npts * ngrp
    cams = camera_slot.shape[0]
    half = cams // 2
    owned = cams // count
    size = obs_point.shape[0]
    tiles = size // LANES
    vmem = pl.BlockSpec(memory_space=pltpu.VMEM)
    hbm = pl.BlockSpec(memory_space=pl.ANY)

    def near(value):
        return pltpu.with_memory_space_constraint(value, pltpu.VMEM)

    mine, theirs, red, last, place = pl.pallas_call(
        terms_kernel,
        in_specs=[vmem] * 4 + [hbm],
        out_specs=[vmem] * 5,
        out_shape=[
            pltpu.VMEM((ROWS, half), jnp.float32),
            pltpu.VMEM((ROWS, half), jnp.float32),
            pltpu.VMEM((8, size), jnp.float32),
            pltpu.VMEM((tiles, LANES), jnp.float32),
            pltpu.VMEM((tiles, LANES), jnp.int32),
        ],
        scratch_shapes=[
            pltpu.VMEM(cam_jac.shape, jnp.float32),
            pltpu.VMEM((8 * tiles, LANES), jnp.float32),
            pltpu.VMEM((16 * tiles, LANES), jnp.float32),
            pltpu.VMEM((5 * tiles, LANES), jnp.float32),
            pltpu.VMEM((tiles, LANES), jnp.float32),
            pltpu.SemaphoreType.DMA,
        ],
        name="terms",
    )(pt_jac, resid, obs_point.reshape(tiles, LANES), obs_camera.reshape(tiles, LANES), cam_jac)

    mate = [(at, at ^ 1) for at in range(count)]
    total = mine + lax.ppermute(theirs, AXES, mate)
    for step in exchange_steps(npts):
        got = [lax.ppermute(total, AXES, partners(count, ngrp, masks)) for masks in step]
        for value in got:
            total = total + value
    theirs = lax.ppermute(total, AXES, mate)

    place, red, last = near(place), near(red), near(last)
    slots = near(camera_slot.reshape(2, half))
    entries = pltpu.VMEM((ROWS * max(8, half // LANES), LANES), jnp.float32)
    own, part, edge = pl.pallas_call(
        functools.partial(first_half_kernel, owned=owned),
        in_specs=[vmem] * 5,
        out_specs=[vmem] * 3,
        out_shape=[
            pltpu.VMEM((ROWS, LANES), jnp.float32),
            pltpu.VMEM((8, size), jnp.float32),
            pltpu.VMEM((tiles, LANES), jnp.float32),
        ],
        scratch_shapes=[entries],
        name="apply_first",
    )(near(total), place, red, last, slots)
    inverse, precond = pl.pallas_call(
        second_half_kernel,
        in_specs=[vmem] * 8,
        out_specs=[hbm, hbm],
        out_shape=[
            jax.ShapeDtypeStruct((owned, 81), jnp.float32),
            jax.ShapeDtypeStruct((9, size), jnp.float32),
        ],
        scratch_shapes=[
            entries,
            pltpu.VMEM((LANES, LANES), jnp.float32),
            pltpu.VMEM((owned, 81), jnp.float32),
            pltpu.VMEM((9, size), jnp.float32),
            pltpu.SemaphoreType.DMA((tiles // GROUP,)),
            pltpu.SemaphoreType.DMA,
        ],
        name="apply_second",
    )(near(theirs), place, red, last, slots, near(own), near(part), near(edge))
    return (inverse.T, precond)


def solution(mesh):
    spread = P(None, AXES)
    in_specs = (spread, spread, spread, P(AXES), P(AXES), P())
    body = functools.partial(shards, npts=mesh.shape["pts"], ngrp=mesh.shape["grp"])
    return jax.shard_map(body, mesh=mesh, in_specs=in_specs, out_specs=(spread, spread), check_vma=False)
```

```python
import functools

import jax
import jax.numpy as jnp
from jax import lax
from jax.experimental import pallas as pl
from jax.experimental.pallas import tpu as pltpu
from jax.sharding import PartitionSpec as P

AXES = ("pts", "grp")
DAMP = 1.0
LANES = 128
ROWS = 48
GROUP = 8
SCATTER = 8


def split3(value):
    high = value.astype(jnp.bfloat16)
    rest = value - high.astype(jnp.float32)
    mid = rest.astype(jnp.bfloat16)
    low = (rest - mid.astype(jnp.float32)).astype(jnp.bfloat16)
    return high, mid, low


def dot_nn(left, right):
    return lax.dot_general(left, right, (((1,), (0,)), ((), ())), preferred_element_type=jnp.float32)


def dot_nt(left, right):
    return lax.dot_general(left, right, (((1,), (1,)), ((), ())), preferred_element_type=jnp.float32)


def row_of(row_at, col_at):
    if row_at == 8 and col_at == 8:
        return 36
    if row_at == 8:
        return 40 + col_at
    if col_at == 8:
        return 40 + row_at
    gap = (col_at - row_at) % 8
    if gap > 4 or (gap == 4 and row_at >= 4):
        return 8 * ((row_at - col_at) % 8) + col_at
    return 8 * gap + row_at


def side_of(device):
    for shift in (8, 4, 2, 1):
        device = device ^ (device >> shift)
    return device & 1


def other_half(named, side, half):
    swapped = jnp.where(named < half, named + half, named - half)
    return jnp.where(side == 0, named, swapped)


def terms_kernel(
    pt_ref, res_ref, point_ref, named_ref, cam_hbm,
    mine_ref, theirs_ref, red_ref, last_ref, place_ref,
    cam_ref, dense_ref, product_ref, total_ref, keep_ref, where_ref, sem,
):
    tiles = point_ref.shape[0]
    pitch = dense_ref.shape[0] // 8
    half = mine_ref.shape[1]
    cams = 2 * half
    load = pltpu.make_async_copy(cam_hbm, cam_ref, sem)
    load.start()
    row = lax.broadcasted_iota(jnp.int32, (8, LANES), 0)
    where_ref[...] = (point_ref[...] - point_ref[0:1, 0:1]).astype(jnp.float32)
    place_ref[...] = other_half(named_ref[...], side_of(lax.axis_index(AXES)), half)
    one = jnp.ones((LANES, LANES), jnp.bfloat16)
    zero_one = jnp.zeros((LANES, LANES), jnp.bfloat16)
    all_columns = []
    all_points = []
    for start in range(0, tiles, GROUP):
        points = where_ref[start : start + GROUP, :]
        both_ids = jnp.concatenate([points, place_ref[start : start + GROUP, :].astype(jnp.float32)], 0)
        all_points.append(points.astype(jnp.int32))
        all_columns.append(jnp.transpose(both_ids).astype(jnp.int32).astype(jnp.int16))

    places = where_ref[...]
    turned = jnp.transpose(places)
    tile_at = lax.broadcasted_iota(jnp.int32, (tiles, tiles), 0)
    other = lax.broadcasted_iota(jnp.int32, (tiles, tiles), 1)
    before = (other < tile_at) & (turned[LANES - 1 : LANES, :] == places[:, 0:1])
    after = (other > tile_at) & (turned[0:1, :] == places[:, LANES - 1 : LANES])
    before = jnp.where(before, 1.0, 0.0).astype(jnp.bfloat16)
    after = jnp.where(after, 1.0, 0.0).astype(jnp.bfloat16)
    head_rows = jnp.where(places == places[:, 0:1], 1.0, 0.0)
    tail_rows = jnp.where(places == places[:, LANES - 1 : LANES], 1.0, 0.0)

    for tile in range(tiles):
        here = slice(tile * LANES, (tile + 1) * LANES)
        dense_ref[pl.ds(tile, 8, stride=pitch), :] = jnp.concatenate([pt_ref[:, here], res_ref[:, here]], 0)
    entries = []
    for start in range(0, tiles, 8):
        top0, top1, top2, low0, low1, low2, res0, res1 = [
            dense_ref[pos * pitch + start : pos * pitch + start + 8, :] for pos in range(8)
        ]
        products = {
            0: top0 * top0 + low0 * low0,
            1: top1 * top1 + low1 * low1,
            2: top2 * top2 + low2 * low2,
            3: top0 * top1 + low0 * low1,
            4: top1 * top2 + low1 * low2,
            5: top0 * top2 + low0 * low2,
            8: top0 * res0 + low0 * res1,
            9: top1 * res0 + low1 * res1,
            10: top2 * res0 + low2 * res1,
        }
        entries.append(products)
        for pos in range(16):
            product_ref[pos * pitch + start : pos * pitch + start + 8, :] = products.get(pos, products[0])

    def gather(tile):
        columns = all_columns[tile // GROUP]
        at = tile % GROUP
        line = jnp.broadcast_to(all_points[tile // GROUP][at : at + 1], (16, LANES)).astype(jnp.int16)
        same = jnp.where(
            jnp.broadcast_to(columns[:, at : at + 1], (LANES, LANES)) == jnp.concatenate([line] * 8, 0),
            one,
            zero_one,
        )
        upper = product_ref[pl.ds(tile, 8, stride=pitch), :]
        lower = product_ref[pl.ds(8 * pitch + tile, 8, stride=pitch), :]
        left = jnp.concatenate(split3(jnp.concatenate([upper, lower], 0)), 0)
        found = dot_nn(left, same)
        found = found[0:16] + found[16:32] + found[32:48]
        total_ref[pl.ds(tile, 8, stride=pitch), :] = found[0:8]
        total_ref[pl.ds(8 * pitch + tile, 8, stride=pitch), :] = found[8:16]

    for tile in range(tiles // 2):
        gather(tile)

    lane8 = lax.broadcasted_iota(jnp.int32, (8, LANES), 1)
    heads = []
    tails = []
    for start in range(0, tiles, 8):
        head = jnp.zeros((8, LANES), jnp.float32)
        tail = jnp.zeros((8, LANES), jnp.float32)
        is_head = head_rows[start : start + 8]
        is_tail = tail_rows[start : start + 8]
        for pos, value in entries[start // 8].items():
            head = jnp.where(lane8 == pos, jnp.sum(value * is_head, axis=1, keepdims=True), head)
            tail = jnp.where(lane8 == pos, jnp.sum(value * is_tail, axis=1, keepdims=True), tail)
        heads.append(head)
        tails.append(tail)

    def carried(matrix, rows):
        parts = [dot_nn(matrix, part) for part in split3(jnp.concatenate(rows, 0))]
        return parts[0] + parts[1] + parts[2]

    from_before = carried(before, tails)
    from_after = carried(after, heads)

    for tile in range(tiles // 2, tiles):
        gather(tile)

    for start in range(0, tiles, 8):
        is_head = head_rows[start : start + 8]
        is_tail = tail_rows[start : start + 8]
        add_before = from_before[start : start + 8]
        add_after = from_after[start : start + 8]

        def total(pos):
            value = total_ref[pos * pitch + start : pos * pitch + start + 8, :]
            return value + is_head * add_before[:, pos : pos + 1] + is_tail * add_after[:, pos : pos + 1]

        v00, v11, v22 = [total(pos) + DAMP for pos in (0, 1, 2)]
        v01, v12, v02 = [total(pos) for pos in (3, 4, 5)]
        bees = [total(pos) for pos in (8, 9, 10)]
        dense = [dense_ref[pos * pitch + start : pos * pitch + start + 8, :] for pos in range(8)]
        c00 = v11 * v22 - v12 * v12
        c01 = v02 * v12 - v01 * v22
        c02 = v01 * v12 - v02 * v11
        c11 = v00 * v22 - v02 * v02
        c12 = v01 * v02 - v00 * v12
        c22 = v00 * v11 - v01 * v01
        scale = 1.0 / (v00 * c00 + v01 * c01 + v02 * c02)
        vinv = [[c00 * scale, c01 * scale, c02 * scale]]
        vinv.append([vinv[0][1], c11 * scale, c12 * scale])
        vinv.append([vinv[0][2], vinv[1][2], c22 * scale])

        def times(vec):
            return [vinv[at][0] * vec[0] + vinv[at][1] * vec[1] + vinv[at][2] * vec[2] for at in range(3)]

        def inner(left, right):
            return left[0] * right[0] + left[1] * right[1] + left[2] * right[2]

        top, low = dense[0:3], dense[3:6]
        use_top, use_low, weight = times(top), times(low), times(bees)
        results = (
            1.0 - inner(top, use_top),
            -inner(top, use_low),
            1.0 - inner(low, use_low),
            dense[6] - inner(top, weight),
            dense[7] - inner(low, weight),
        )
        for pos, value in enumerate(results):
            keep_ref[pos * tiles + start : pos * tiles + start + 8, :] = value

    load.wait()
    lane16 = lax.broadcasted_iota(jnp.int32, (16, LANES), 1)
    names = [(lane16 + at * LANES).astype(jnp.int16) for at in range(cams // LANES)]
    one = jnp.ones((16, LANES), jnp.bfloat16)
    zero_one = jnp.zeros((16, LANES), jnp.bfloat16)
    acc = jnp.zeros((3 * ROWS, cams), jnp.float32)
    for start in range(0, tiles, SCATTER):
        lefts = []
        rights = []
        for tile in range(start, start + SCATTER):
            here = slice(tile * LANES, (tile + 1) * LANES)

            def spread(ref, at):
                return ref[pl.ds(at, 8, stride=0), :]

            k00, k01, k11, s0, s1 = [spread(keep_ref, pos * tiles + tile) for pos in range(5)]
            zero, one_row = cam_ref[0:8, here], cam_ref[9:17, here]
            zero8 = jnp.broadcast_to(cam_ref[8:9, here], (8, LANES))
            one8 = jnp.broadcast_to(cam_ref[17:18, here], (8, LANES))
            m0 = k00 * zero + k01 * one_row
            m1 = k01 * zero + k11 * one_row
            corner = zero8 * (k00 * zero8 + k01 * one8) + one8 * (k01 * zero8 + k11 * one8)
            pieces = [zero * m0 + one_row * m1]
            for gap in range(1, 5):
                pieces.append(zero * pltpu.roll(m0, 8 - gap, 0) + one_row * pltpu.roll(m1, 8 - gap, 0))
            pieces[4] = jnp.where(row == 4, corner, pieces[4])
            pieces.append(zero8 * m0 + one8 * m1)
            lefts.append(jnp.concatenate(split3(jnp.concatenate(pieces, 0)), 0))
            red_ref[:, here] = zero * s0 + one_row * s1
            last_ref[tile : tile + 1, :] = (zero8 * s0 + one8 * s1)[0:1]
            source = all_columns[tile // GROUP]
            column_at = GROUP + tile % GROUP
            for at in range(0, LANES, 16):
                column = jnp.broadcast_to(source[at : at + 16, column_at : column_at + 1], (16, LANES))
                rights.append(jnp.concatenate([jnp.where(column == name, one, zero_one) for name in names], 1))
        acc = acc + dot_nn(jnp.concatenate(lefts, 1), jnp.concatenate(rights, 0))
    done = acc[0:ROWS] + acc[ROWS : 2 * ROWS] + acc[2 * ROWS : 3 * ROWS]
    mine_ref[...] = done[:, 0:half]
    theirs_ref[...] = done[:, half:cams]


def inverse_of(entry):
    entry = dict(entry)
    root = {}
    factor = {}
    for col_at in range(9):
        root[col_at] = lax.rsqrt(entry[col_at, col_at])
        for row_at in range(col_at + 1, 9):
            factor[row_at, col_at] = entry[row_at, col_at] * root[col_at]
        for row_at in range(col_at + 1, 9):
            for inner in range(col_at + 1, row_at + 1):
                entry[row_at, inner] = entry[row_at, inner] - factor[row_at, col_at] * factor[inner, col_at]
    solved = {}
    for col_at in range(9):
        solved[col_at, col_at] = root[col_at]
        for row_at in range(col_at + 1, 9):
            value = factor[row_at, col_at] * solved[col_at, col_at]
            for inner in range(col_at + 1, row_at):
                value = value + factor[row_at, inner] * solved[inner, col_at]
            solved[row_at, col_at] = -value * root[row_at]
    result = {}
    for row_at in range(9):
        for col_at in range(row_at + 1):
            value = solved[row_at, row_at] * solved[row_at, col_at]
            for inner in range(row_at + 1, 9):
                value = value + solved[inner, row_at] * solved[inner, col_at]
            result[row_at, col_at] = value
    return result


def inverse_table(source_ref, entry_ref):
    half = source_ref.shape[1]
    cols = half // LANES
    step_rows = entry_ref.shape[0] // ROWS
    for block in range(ROWS // 8):
        for col in range(cols):
            entry_ref[pl.ds(block * 8 * step_rows + col, 8, stride=step_rows), :] = source_ref[
                block * 8 : block * 8 + 8, col * LANES : (col + 1) * LANES
            ]

    def entry_at(row_at, col_at):
        at = row_of(row_at, col_at) * step_rows
        return entry_ref[at : at + cols, :]

    entry = {(r, c): entry_at(r, c) for r in range(9) for c in range(r + 1)}
    for at in range(9):
        entry[at, at] = entry[at, at] + DAMP
    result = inverse_of(entry)
    spare = jnp.zeros((cols, LANES), jnp.float32)
    for at in (37, 38, 39):
        entry_ref[at * step_rows : at * step_rows + cols, :] = spare
    for (row_at, col_at), value in result.items():
        at = row_of(row_at, col_at) * step_rows
        entry_ref[at : at + cols, :] = value
    tables = []
    for col in range(cols):
        blocks = [
            entry_ref[pl.ds(block * 8 * step_rows + col, 8, stride=step_rows), :] for block in range(ROWS // 8)
        ]
        tables.append(jnp.concatenate(split3(jnp.concatenate(blocks, 0)), 0))
    return jnp.concatenate(tables, 1)


def add_parts(found):
    return found[0:ROWS] + found[ROWS : 2 * ROWS] + found[2 * ROWS : 3 * ROWS]


def owned_columns(table, slot_ref, at, owned):
    want = lax.broadcasted_iota(jnp.int32, (LANES, slot_ref.shape[1]), 0) + lax.axis_index(AXES) * owned
    pick = jnp.where(slot_ref[pl.ds(at, 1), :] == want, 1.0, 0.0).astype(jnp.bfloat16)
    return add_parts(dot_nt(table, pick))


def applied(table, place_ref, red_ref, last_ref, first, start):
    half = table.shape[1]
    row = lax.broadcasted_iota(jnp.int32, (8, LANES), 0)
    row16 = lax.broadcasted_iota(jnp.int32, (16, LANES), 0) + first
    one = jnp.ones((16, LANES), jnp.bfloat16)
    zero_one = jnp.zeros((16, LANES), jnp.bfloat16)
    rights = []
    for tile in range(start, start + GROUP):
        gap = (place_ref[pl.ds(tile, 16, stride=0), :] - row16).astype(jnp.int16)
        rights.append(
            jnp.concatenate([jnp.where(gap == jnp.int16(at), one, zero_one) for at in range(0, half, 16)], 0)
        )
    found = add_parts(dot_nn(table, jnp.concatenate(rights, 1)))
    results = []
    for at in range(GROUP):
        tile = start + at
        here = slice(tile * LANES, (tile + 1) * LANES)
        block = [found[8 * pos : 8 * pos + 8, at * LANES : (at + 1) * LANES] for pos in range(6)]
        red = red_ref[:, here]
        last = last_ref[pl.ds(tile, 8, stride=0), :]
        whole = jnp.where(row < 4, block[4], pltpu.roll(block[4], 4, 0))
        value = block[0] * red + block[5] * last + whole * pltpu.roll(red, 4, 0)
        for gap in range(1, 4):
            value = value + block[gap] * pltpu.roll(red, 8 - gap, 0)
            value = value + pltpu.roll(block[gap] * red, gap, 0)
        edge = jnp.sum(block[5] * red, axis=0, keepdims=True)
        results.append((tile, here, value, edge + (block[4] * last)[4:5]))
    return results


def first_half_kernel(
    mine_ref, place_ref, red_ref, last_ref, slot_ref,
    own_ref, part_ref, edge_ref,
    entry_ref, *, owned,
):
    table = inverse_table(mine_ref, entry_ref)
    for start in range(0, place_ref.shape[0], GROUP):
        for tile, here, value, edge in applied(table, place_ref, red_ref, last_ref, 0, start):
            part_ref[:, here] = value
            edge_ref[tile : tile + 1, :] = edge
    own_ref[...] = owned_columns(table, slot_ref, side_of(lax.axis_index(AXES)), owned)


def second_half_kernel(
    theirs_ref, place_ref, red_ref, last_ref, slot_ref, own_ref, part_ref, edge_ref,
    inv_hbm, out_hbm,
    entry_ref, square_ref, turned_ref, out_ref, sems, own_sem,
):
    tiles, half = place_ref.shape[0], theirs_ref.shape[1]
    owned = inv_hbm.shape[0]
    table = inverse_table(theirs_ref, entry_ref)
    own = own_ref[...] + owned_columns(table, slot_ref, 1 - side_of(lax.axis_index(AXES)), owned)
    square_ref[81:LANES, :] = jnp.zeros((LANES - 81, LANES), jnp.float32)
    for row_at in range(9):
        for col_at in range(9):
            at = row_of(row_at, col_at)
            square_ref[row_at * 9 + col_at : row_at * 9 + col_at + 1, :] = own[at : at + 1]
    turned_ref[...] = jnp.transpose(square_ref[...])[0:owned, 0:81]
    own_copy = pltpu.make_async_copy(turned_ref, inv_hbm, own_sem)
    own_copy.start()
    copies = []
    for start in range(0, tiles, GROUP):
        for tile, here, value, edge in applied(table, place_ref, red_ref, last_ref, half, start):
            out_ref[0:8, here] = value + part_ref[:, here]
            out_ref[8:9, here] = edge + edge_ref[tile : tile + 1, :]
        span = pl.ds(start * LANES, GROUP * LANES)
        copy = pltpu.make_async_copy(out_ref.at[:, span], out_hbm.at[:, span], sems.at[start // GROUP])
        copy.start()
        copies.append(copy)
    own_copy.wait()
    for copy in copies:
        copy.wait()


def partners(count, ngrp, masks):
    pairs = []
    for at in range(count):
        mask = masks[at.bit_count() % 2]
        pairs.append((at, at ^ (mask * ngrp + mask.bit_count() % 2)))
    return pairs


def exchange_steps(npts):
    bits = [1 << at for at in range(npts.bit_length() - 1)]
    pairs = [(bits[at], bits[at + 1], bits[at] + bits[at + 1]) for at in range(0, len(bits) - 1, 2)]
    turned = pairs[1:] + pairs[:1]
    steps = [list(zip(one, two)) for one, two in zip(pairs, turned)]
    if len(bits) % 2 == 1:
        steps.append([(bits[-1], bits[-1])])
    return steps


def shards(cam_jac, pt_jac, resid, obs_point, obs_camera, camera_slot, *, npts, ngrp):
    count = npts * ngrp
    cams = camera_slot.shape[0]
    half = cams // 2
    owned = cams // count
    size = obs_point.shape[0]
    tiles = size // LANES
    vmem = pl.BlockSpec(memory_space=pltpu.VMEM)
    hbm = pl.BlockSpec(memory_space=pl.ANY)

    def near(value):
        return pltpu.with_memory_space_constraint(value, pltpu.VMEM)

    mine, theirs, red, last, place = pl.pallas_call(
        terms_kernel,
        in_specs=[vmem] * 4 + [hbm],
        out_specs=[vmem] * 5,
        out_shape=[
            pltpu.VMEM((ROWS, half), jnp.float32),
            pltpu.VMEM((ROWS, half), jnp.float32),
            pltpu.VMEM((8, size), jnp.float32),
            pltpu.VMEM((tiles, LANES), jnp.float32),
            pltpu.VMEM((tiles, LANES), jnp.int32),
        ],
        scratch_shapes=[
            pltpu.VMEM(cam_jac.shape, jnp.float32),
            pltpu.VMEM((8 * (tiles + 8), LANES), jnp.float32),
            pltpu.VMEM((16 * (tiles + 8), LANES), jnp.float32),
            pltpu.VMEM((16 * (tiles + 8), LANES), jnp.float32),
            pltpu.VMEM((5 * tiles, LANES), jnp.float32),
            pltpu.VMEM((tiles, LANES), jnp.float32),
            pltpu.SemaphoreType.DMA,
        ],
        name="terms",
    )(pt_jac, resid, obs_point.reshape(tiles, LANES), obs_camera.reshape(tiles, LANES), cam_jac)

    mate = [(at, at ^ 1) for at in range(count)]
    total = mine + lax.ppermute(theirs, AXES, mate)
    for step in exchange_steps(npts):
        got = [lax.ppermute(total, AXES, partners(count, ngrp, masks)) for masks in step]
        for value in got:
            total = total + value
    theirs = lax.ppermute(total, AXES, mate)

    place, red, last = near(place), near(red), near(last)
    slots = near(camera_slot.reshape(2, half))
    entries = pltpu.VMEM((ROWS * max(8, half // LANES), LANES), jnp.float32)
    own, part, edge = pl.pallas_call(
        functools.partial(first_half_kernel, owned=owned),
        in_specs=[vmem] * 5,
        out_specs=[vmem] * 3,
        out_shape=[
            pltpu.VMEM((ROWS, LANES), jnp.float32),
            pltpu.VMEM((8, size), jnp.float32),
            pltpu.VMEM((tiles, LANES), jnp.float32),
        ],
        scratch_shapes=[entries],
        name="apply_first",
    )(near(total), place, red, last, slots)
    inverse, precond = pl.pallas_call(
        second_half_kernel,
        in_specs=[vmem] * 8,
        out_specs=[hbm, hbm],
        out_shape=[
            jax.ShapeDtypeStruct((owned, 81), jnp.float32),
            jax.ShapeDtypeStruct((9, size), jnp.float32),
        ],
        scratch_shapes=[
            entries,
            pltpu.VMEM((LANES, LANES), jnp.float32),
            pltpu.VMEM((owned, 81), jnp.float32),
            pltpu.VMEM((9, size), jnp.float32),
            pltpu.SemaphoreType.DMA((tiles // GROUP,)),
            pltpu.SemaphoreType.DMA,
        ],
        name="apply_second",
    )(near(theirs), place, red, last, slots, near(own), near(part), near(edge))
    return (inverse.T, precond)


def solution(mesh):
    spread = P(None, AXES)
    in_specs = (spread, spread, spread, P(AXES), P(AXES), P())
    body = functools.partial(shards, npts=mesh.shape["pts"], ngrp=mesh.shape["grp"])
    return jax.shard_map(body, mesh=mesh, in_specs=in_specs, out_specs=(spread, spread), check_vma=False)
```

```python
import functools

import jax
import jax.numpy as jnp
from jax import lax
from jax.experimental import pallas as pl
from jax.experimental.pallas import tpu as pltpu
from jax.sharding import PartitionSpec as P

AXES = ("pts", "grp")
DAMP = 1.0
LANES = 128
ROWS = 48
GROUP = 8
SCATTER = 8


def split3(value):
    high = value.astype(jnp.bfloat16)
    rest = value - high.astype(jnp.float32)
    mid = rest.astype(jnp.bfloat16)
    low = (rest - mid.astype(jnp.float32)).astype(jnp.bfloat16)
    return high, mid, low


def dot_nn(left, right):
    return lax.dot_general(left, right, (((1,), (0,)), ((), ())), preferred_element_type=jnp.float32)


def dot_nt(left, right):
    return lax.dot_general(left, right, (((1,), (1,)), ((), ())), preferred_element_type=jnp.float32)


def row_of(row_at, col_at):
    if row_at == 8 and col_at == 8:
        return 36
    if row_at == 8:
        return 40 + col_at
    if col_at == 8:
        return 40 + row_at
    gap = (col_at - row_at) % 8
    if gap > 4 or (gap == 4 and row_at >= 4):
        return 8 * ((row_at - col_at) % 8) + col_at
    return 8 * gap + row_at


def side_of(device):
    for shift in (8, 4, 2, 1):
        device = device ^ (device >> shift)
    return device & 1


def other_half(named, side, half):
    swapped = jnp.where(named < half, named + half, named - half)
    return jnp.where(side == 0, named, swapped)


def terms_kernel(
    pt_ref, res_ref, point_ref, named_ref, cam_hbm,
    mine_ref, theirs_ref, red_ref, last_ref, place_ref,
    cam_ref, dense_ref, product_ref, total_ref, edge_ref, corner_ref, keep_ref, where_ref, sem,
):
    tiles = point_ref.shape[0]
    pitch = dense_ref.shape[0] // 8
    half = mine_ref.shape[1]
    cams = 2 * half
    load = pltpu.make_async_copy(cam_hbm, cam_ref, sem)
    load.start()
    row = lax.broadcasted_iota(jnp.int32, (8, LANES), 0)
    where_ref[...] = (point_ref[...] - point_ref[0:1, 0:1]).astype(jnp.float32)
    place_ref[...] = other_half(named_ref[...], side_of(lax.axis_index(AXES)), half)
    one = jnp.ones((LANES, LANES), jnp.bfloat16)
    zero_one = jnp.zeros((LANES, LANES), jnp.bfloat16)
    all_columns = []
    all_points = []
    for start in range(0, tiles, GROUP):
        points = where_ref[start : start + GROUP, :]
        both_ids = jnp.concatenate([points, place_ref[start : start + GROUP, :].astype(jnp.float32)], 0)
        all_points.append(points.astype(jnp.int32))
        all_columns.append(jnp.transpose(both_ids).astype(jnp.int32).astype(jnp.int16))

    places = where_ref[...]
    turned = jnp.transpose(places)
    tile_at = lax.broadcasted_iota(jnp.int32, (tiles, tiles), 0)
    other = lax.broadcasted_iota(jnp.int32, (tiles, tiles), 1)
    before = (other < tile_at) & (turned[LANES - 1 : LANES, :] == places[:, 0:1])
    after = (other > tile_at) & (turned[0:1, :] == places[:, LANES - 1 : LANES])
    before = jnp.where(before, 1.0, 0.0).astype(jnp.bfloat16)
    after = jnp.where(after, 1.0, 0.0).astype(jnp.bfloat16)
    head_rows = jnp.where(places == places[:, 0:1], 1.0, 0.0)
    tail_rows = jnp.where(places == places[:, LANES - 1 : LANES], 1.0, 0.0)

    for tile in range(tiles):
        here = slice(tile * LANES, (tile + 1) * LANES)
        dense_ref[pl.ds(tile, 8, stride=pitch), :] = jnp.concatenate([pt_ref[:, here], res_ref[:, here]], 0)
    entries = []
    for start in range(0, tiles, 8):
        top0, top1, top2, low0, low1, low2, res0, res1 = [
            dense_ref[pos * pitch + start : pos * pitch + start + 8, :] for pos in range(8)
        ]
        products = {
            0: top0 * top0 + low0 * low0,
            1: top1 * top1 + low1 * low1,
            2: top2 * top2 + low2 * low2,
            3: top0 * top1 + low0 * low1,
            4: top1 * top2 + low1 * low2,
            5: top0 * top2 + low0 * low2,
            8: top0 * res0 + low0 * res1,
            9: top1 * res0 + low1 * res1,
            10: top2 * res0 + low2 * res1,
        }
        entries.append(products)
        for pos in range(16):
            product_ref[pos * pitch + start : pos * pitch + start + 8, :] = products.get(pos, products[0])

    def gather(tile):
        columns = all_columns[tile // GROUP]
        at = tile % GROUP
        line = jnp.broadcast_to(all_points[tile // GROUP][at : at + 1], (16, LANES)).astype(jnp.int16)
        same = jnp.where(
            jnp.broadcast_to(columns[:, at : at + 1], (LANES, LANES)) == jnp.concatenate([line] * 8, 0),
            one,
            zero_one,
        )
        upper = product_ref[pl.ds(tile, 8, stride=pitch), :]
        lower = product_ref[pl.ds(8 * pitch + tile, 8, stride=pitch), :]
        left = jnp.concatenate(split3(jnp.concatenate([upper, lower], 0)), 0)
        found = dot_nn(left, same)
        found = found[0:16] + found[16:32] + found[32:48]
        total_ref[pl.ds(tile, 8, stride=pitch), :] = found[0:8]
        total_ref[pl.ds(8 * pitch + tile, 8, stride=pitch), :] = found[8:16]

    for tile in range(tiles // 2):
        gather(tile)

    lane8 = lax.broadcasted_iota(jnp.int32, (8, LANES), 1)
    heads = []
    tails = []
    for start in range(0, tiles, 8):
        head = jnp.zeros((8, LANES), jnp.float32)
        tail = jnp.zeros((8, LANES), jnp.float32)
        is_head = head_rows[start : start + 8]
        is_tail = tail_rows[start : start + 8]
        for pos, value in entries[start // 8].items():
            head = jnp.where(lane8 == pos, jnp.sum(value * is_head, axis=1, keepdims=True), head)
            tail = jnp.where(lane8 == pos, jnp.sum(value * is_tail, axis=1, keepdims=True), tail)
        heads.append(head)
        tails.append(tail)

    def carried(matrix, rows):
        parts = [dot_nn(matrix, part) for part in split3(jnp.concatenate(rows, 0))]
        return parts[0] + parts[1] + parts[2]

    from_before = carried(before, tails)
    from_after = carried(after, heads)

    for tile in range(tiles // 2, tiles):
        gather(tile)

    for start in range(0, tiles, 8):
        is_head = head_rows[start : start + 8]
        is_tail = tail_rows[start : start + 8]
        add_before = from_before[start : start + 8]
        add_after = from_after[start : start + 8]

        def total(pos):
            value = total_ref[pos * pitch + start : pos * pitch + start + 8, :]
            return value + is_head * add_before[:, pos : pos + 1] + is_tail * add_after[:, pos : pos + 1]

        v00, v11, v22 = [total(pos) + DAMP for pos in (0, 1, 2)]
        v01, v12, v02 = [total(pos) for pos in (3, 4, 5)]
        bees = [total(pos) for pos in (8, 9, 10)]
        dense = [dense_ref[pos * pitch + start : pos * pitch + start + 8, :] for pos in range(8)]
        c00 = v11 * v22 - v12 * v12
        c01 = v02 * v12 - v01 * v22
        c02 = v01 * v12 - v02 * v11
        c11 = v00 * v22 - v02 * v02
        c12 = v01 * v02 - v00 * v12
        c22 = v00 * v11 - v01 * v01
        scale = 1.0 / (v00 * c00 + v01 * c01 + v02 * c02)
        vinv = [[c00 * scale, c01 * scale, c02 * scale]]
        vinv.append([vinv[0][1], c11 * scale, c12 * scale])
        vinv.append([vinv[0][2], vinv[1][2], c22 * scale])

        def times(vec):
            return [vinv[at][0] * vec[0] + vinv[at][1] * vec[1] + vinv[at][2] * vec[2] for at in range(3)]

        def inner(left, right):
            return left[0] * right[0] + left[1] * right[1] + left[2] * right[2]

        top, low = dense[0:3], dense[3:6]
        use_top, use_low, weight = times(top), times(low), times(bees)
        results = (
            1.0 - inner(top, use_top),
            -inner(top, use_low),
            1.0 - inner(low, use_low),
            dense[6] - inner(top, weight),
            dense[7] - inner(low, weight),
        )
        for pos, value in enumerate(results):
            keep_ref[pos * tiles + start : pos * tiles + start + 8, :] = value

    load.wait()
    for tile in range(tiles):
        here = slice(tile * LANES, (tile + 1) * LANES)
        edge_ref[pl.ds(tile, 8, stride=pitch), :] = cam_ref[8:16, here]
        edge_ref[pl.ds(8 * pitch + tile, 2, stride=pitch), :] = cam_ref[16:18, here]
    for start in range(0, tiles, 8):
        here = slice(start, start + 8)
        zero8 = edge_ref[here, :]
        one8 = edge_ref[9 * pitch + start : 9 * pitch + start + 8, :]
        k00, k01, k11, s0, s1 = [keep_ref[pos * tiles + start : pos * tiles + start + 8, :] for pos in range(5)]
        corner_ref[here, :] = zero8 * (k00 * zero8 + k01 * one8) + one8 * (k01 * zero8 + k11 * one8)
        last_ref[here, :] = zero8 * s0 + one8 * s1
    lane16 = lax.broadcasted_iota(jnp.int32, (16, LANES), 1)
    names = [(lane16 + at * LANES).astype(jnp.int16) for at in range(cams // LANES)]
    one = jnp.ones((16, LANES), jnp.bfloat16)
    zero_one = jnp.zeros((16, LANES), jnp.bfloat16)
    acc = jnp.zeros((3 * ROWS, cams), jnp.float32)
    for start in range(0, tiles, SCATTER):
        lefts = []
        rights = []
        for tile in range(start, start + SCATTER):
            here = slice(tile * LANES, (tile + 1) * LANES)

            def spread(ref, at):
                return ref[pl.ds(at, 8, stride=0), :]

            k00, k01, k11, s0, s1 = [spread(keep_ref, pos * tiles + tile) for pos in range(5)]
            zero = cam_ref[0:8, here]
            one_row = edge_ref[pl.ds(pitch + tile, 8, stride=pitch), :]
            zero8 = spread(edge_ref, tile)
            one8 = spread(edge_ref, 9 * pitch + tile)
            m0 = k00 * zero + k01 * one_row
            m1 = k01 * zero + k11 * one_row
            corner = spread(corner_ref, tile)
            pieces = [zero * m0 + one_row * m1]
            for gap in range(1, 5):
                pieces.append(zero * pltpu.roll(m0, 8 - gap, 0) + one_row * pltpu.roll(m1, 8 - gap, 0))
            pieces[4] = jnp.where(row == 4, corner, pieces[4])
            pieces.append(zero8 * m0 + one8 * m1)
            lefts.append(jnp.concatenate(split3(jnp.concatenate(pieces, 0)), 0))
            red_ref[:, here] = zero * s0 + one_row * s1
            source = all_columns[tile // GROUP]
            column_at = GROUP + tile % GROUP
            for at in range(0, LANES, 16):
                column = jnp.broadcast_to(source[at : at + 16, column_at : column_at + 1], (16, LANES))
                rights.append(jnp.concatenate([jnp.where(column == name, one, zero_one) for name in names], 1))
        acc = acc + dot_nn(jnp.concatenate(lefts, 1), jnp.concatenate(rights, 0))
    done = acc[0:ROWS] + acc[ROWS : 2 * ROWS] + acc[2 * ROWS : 3 * ROWS]
    mine_ref[...] = done[:, 0:half]
    theirs_ref[...] = done[:, half:cams]


def inverse_of(entry):
    entry = dict(entry)
    root = {}
    factor = {}
    for col_at in range(9):
        root[col_at] = lax.rsqrt(entry[col_at, col_at])
        for row_at in range(col_at + 1, 9):
            factor[row_at, col_at] = entry[row_at, col_at] * root[col_at]
        for row_at in range(col_at + 1, 9):
            for inner in range(col_at + 1, row_at + 1):
                entry[row_at, inner] = entry[row_at, inner] - factor[row_at, col_at] * factor[inner, col_at]
    solved = {}
    for col_at in range(9):
        solved[col_at, col_at] = root[col_at]
        for row_at in range(col_at + 1, 9):
            value = factor[row_at, col_at] * solved[col_at, col_at]
            for inner in range(col_at + 1, row_at):
                value = value + factor[row_at, inner] * solved[inner, col_at]
            solved[row_at, col_at] = -value * root[row_at]
    result = {}
    for row_at in range(9):
        for col_at in range(row_at + 1):
            value = solved[row_at, row_at] * solved[row_at, col_at]
            for inner in range(row_at + 1, 9):
                value = value + solved[inner, row_at] * solved[inner, col_at]
            result[row_at, col_at] = value
    return result


def inverse_table(source_ref, entry_ref):
    half = source_ref.shape[1]
    cols = half // LANES
    step_rows = entry_ref.shape[0] // ROWS
    for block in range(ROWS // 8):
        for col in range(cols):
            entry_ref[pl.ds(block * 8 * step_rows + col, 8, stride=step_rows), :] = source_ref[
                block * 8 : block * 8 + 8, col * LANES : (col + 1) * LANES
            ]

    def entry_at(row_at, col_at):
        at = row_of(row_at, col_at) * step_rows
        return entry_ref[at : at + cols, :]

    entry = {(r, c): entry_at(r, c) for r in range(9) for c in range(r + 1)}
    for at in range(9):
        entry[at, at] = entry[at, at] + DAMP
    result = inverse_of(entry)
    spare = jnp.zeros((cols, LANES), jnp.float32)
    for at in (37, 38, 39):
        entry_ref[at * step_rows : at * step_rows + cols, :] = spare
    for (row_at, col_at), value in result.items():
        at = row_of(row_at, col_at) * step_rows
        entry_ref[at : at + cols, :] = value
    tables = []
    for col in range(cols):
        blocks = [
            entry_ref[pl.ds(block * 8 * step_rows + col, 8, stride=step_rows), :] for block in range(ROWS // 8)
        ]
        tables.append(jnp.concatenate(split3(jnp.concatenate(blocks, 0)), 0))
    return jnp.concatenate(tables, 1)


def add_parts(found):
    return found[0:ROWS] + found[ROWS : 2 * ROWS] + found[2 * ROWS : 3 * ROWS]


def owned_columns(table, slot_ref, at, owned):
    want = lax.broadcasted_iota(jnp.int32, (LANES, slot_ref.shape[1]), 0) + lax.axis_index(AXES) * owned
    pick = jnp.where(slot_ref[pl.ds(at, 1), :] == want, 1.0, 0.0).astype(jnp.bfloat16)
    return add_parts(dot_nt(table, pick))


def applied(table, place_ref, red_ref, last_ref, first, start):
    half = table.shape[1]
    row = lax.broadcasted_iota(jnp.int32, (8, LANES), 0)
    row16 = lax.broadcasted_iota(jnp.int32, (16, LANES), 0) + first
    one = jnp.ones((16, LANES), jnp.bfloat16)
    zero_one = jnp.zeros((16, LANES), jnp.bfloat16)
    rights = []
    for tile in range(start, start + GROUP):
        gap = (place_ref[pl.ds(tile, 16, stride=0), :] - row16).astype(jnp.int16)
        rights.append(
            jnp.concatenate([jnp.where(gap == jnp.int16(at), one, zero_one) for at in range(0, half, 16)], 0)
        )
    found = add_parts(dot_nn(table, jnp.concatenate(rights, 1)))
    results = []
    for at in range(GROUP):
        tile = start + at
        here = slice(tile * LANES, (tile + 1) * LANES)
        block = [found[8 * pos : 8 * pos + 8, at * LANES : (at + 1) * LANES] for pos in range(6)]
        red = red_ref[:, here]
        last = last_ref[pl.ds(tile, 8, stride=0), :]
        whole = jnp.where(row < 4, block[4], pltpu.roll(block[4], 4, 0))
        value = block[0] * red + block[5] * last + whole * pltpu.roll(red, 4, 0)
        for gap in range(1, 4):
            value = value + block[gap] * pltpu.roll(red, 8 - gap, 0)
            value = value + pltpu.roll(block[gap] * red, gap, 0)
        edge = jnp.sum(block[5] * red, axis=0, keepdims=True)
        results.append((tile, here, value, edge + (block[4] * last)[4:5]))
    return results


def first_half_kernel(
    mine_ref, place_ref, red_ref, last_ref, slot_ref,
    own_ref, part_ref, edge_ref,
    entry_ref, *, owned,
):
    table = inverse_table(mine_ref, entry_ref)
    for start in range(0, place_ref.shape[0], GROUP):
        for tile, here, value, edge in applied(table, place_ref, red_ref, last_ref, 0, start):
            part_ref[:, here] = value
            edge_ref[tile : tile + 1, :] = edge
    own_ref[...] = owned_columns(table, slot_ref, side_of(lax.axis_index(AXES)), owned)


def second_half_kernel(
    theirs_ref, place_ref, red_ref, last_ref, slot_ref, own_ref, part_ref, edge_ref,
    inv_hbm, out_hbm,
    entry_ref, square_ref, turned_ref, out_ref, sems, own_sem,
):
    tiles, half = place_ref.shape[0], theirs_ref.shape[1]
    owned = inv_hbm.shape[0]
    table = inverse_table(theirs_ref, entry_ref)
    own = own_ref[...] + owned_columns(table, slot_ref, 1 - side_of(lax.axis_index(AXES)), owned)
    square_ref[81:LANES, :] = jnp.zeros((LANES - 81, LANES), jnp.float32)
    for row_at in range(9):
        for col_at in range(9):
            at = row_of(row_at, col_at)
            square_ref[row_at * 9 + col_at : row_at * 9 + col_at + 1, :] = own[at : at + 1]
    turned_ref[...] = jnp.transpose(square_ref[...])[0:owned, 0:81]
    own_copy = pltpu.make_async_copy(turned_ref, inv_hbm, own_sem)
    own_copy.start()
    copies = []
    for start in range(0, tiles, GROUP):
        for tile, here, value, edge in applied(table, place_ref, red_ref, last_ref, half, start):
            out_ref[0:8, here] = value + part_ref[:, here]
            out_ref[8:9, here] = edge + edge_ref[tile : tile + 1, :]
        span = pl.ds(start * LANES, GROUP * LANES)
        copy = pltpu.make_async_copy(out_ref.at[:, span], out_hbm.at[:, span], sems.at[start // GROUP])
        copy.start()
        copies.append(copy)
    own_copy.wait()
    for copy in copies:
        copy.wait()


def partners(count, ngrp, masks):
    pairs = []
    for at in range(count):
        mask = masks[at.bit_count() % 2]
        pairs.append((at, at ^ (mask * ngrp + mask.bit_count() % 2)))
    return pairs


def exchange_steps(npts):
    bits = [1 << at for at in range(npts.bit_length() - 1)]
    pairs = [(bits[at], bits[at + 1], bits[at] + bits[at + 1]) for at in range(0, len(bits) - 1, 2)]
    turned = pairs[1:] + pairs[:1]
    steps = [list(zip(one, two)) for one, two in zip(pairs, turned)]
    if len(bits) % 2 == 1:
        steps.append([(bits[-1], bits[-1])])
    return steps


def shards(cam_jac, pt_jac, resid, obs_point, obs_camera, camera_slot, *, npts, ngrp):
    count = npts * ngrp
    cams = camera_slot.shape[0]
    half = cams // 2
    owned = cams // count
    size = obs_point.shape[0]
    tiles = size // LANES
    vmem = pl.BlockSpec(memory_space=pltpu.VMEM)
    hbm = pl.BlockSpec(memory_space=pl.ANY)

    def near(value):
        return pltpu.with_memory_space_constraint(value, pltpu.VMEM)

    mine, theirs, red, last, place = pl.pallas_call(
        terms_kernel,
        in_specs=[vmem] * 4 + [hbm],
        out_specs=[vmem] * 5,
        out_shape=[
            pltpu.VMEM((ROWS, half), jnp.float32),
            pltpu.VMEM((ROWS, half), jnp.float32),
            pltpu.VMEM((8, size), jnp.float32),
            pltpu.VMEM((tiles, LANES), jnp.float32),
            pltpu.VMEM((tiles, LANES), jnp.int32),
        ],
        scratch_shapes=[
            pltpu.VMEM(cam_jac.shape, jnp.float32),
            pltpu.VMEM((8 * (tiles + 8), LANES), jnp.float32),
            pltpu.VMEM((16 * (tiles + 8), LANES), jnp.float32),
            pltpu.VMEM((16 * (tiles + 8), LANES), jnp.float32),
            pltpu.VMEM((10 * (tiles + 8), LANES), jnp.float32),
            pltpu.VMEM((tiles, LANES), jnp.float32),
            pltpu.VMEM((5 * tiles, LANES), jnp.float32),
            pltpu.VMEM((tiles, LANES), jnp.float32),
            pltpu.SemaphoreType.DMA,
        ],
        name="terms",
    )(pt_jac, resid, obs_point.reshape(tiles, LANES), obs_camera.reshape(tiles, LANES), cam_jac)

    mate = [(at, at ^ 1) for at in range(count)]
    total = mine + lax.ppermute(theirs, AXES, mate)
    for step in exchange_steps(npts):
        got = [lax.ppermute(total, AXES, partners(count, ngrp, masks)) for masks in step]
        for value in got:
            total = total + value
    theirs = lax.ppermute(total, AXES, mate)

    place, red, last = near(place), near(red), near(last)
    slots = near(camera_slot.reshape(2, half))
    entries = pltpu.VMEM((ROWS * max(8, half // LANES), LANES), jnp.float32)
    own, part, edge = pl.pallas_call(
        functools.partial(first_half_kernel, owned=owned),
        in_specs=[vmem] * 5,
        out_specs=[vmem] * 3,
        out_shape=[
            pltpu.VMEM((ROWS, LANES), jnp.float32),
            pltpu.VMEM((8, size), jnp.float32),
            pltpu.VMEM((tiles, LANES), jnp.float32),
        ],
        scratch_shapes=[entries],
        name="apply_first",
    )(near(total), place, red, last, slots)
    inverse, precond = pl.pallas_call(
        second_half_kernel,
        in_specs=[vmem] * 8,
        out_specs=[hbm, hbm],
        out_shape=[
            jax.ShapeDtypeStruct((owned, 81), jnp.float32),
            jax.ShapeDtypeStruct((9, size), jnp.float32),
        ],
        scratch_shapes=[
            entries,
            pltpu.VMEM((LANES, LANES), jnp.float32),
            pltpu.VMEM((owned, 81), jnp.float32),
            pltpu.VMEM((9, size), jnp.float32),
            pltpu.SemaphoreType.DMA((tiles // GROUP,)),
            pltpu.SemaphoreType.DMA,
        ],
        name="apply_second",
    )(near(theirs), place, red, last, slots, near(own), near(part), near(edge))
    return (inverse.T, precond)


def solution(mesh):
    spread = P(None, AXES)
    in_specs = (spread, spread, spread, P(AXES), P(AXES), P())
    body = functools.partial(shards, npts=mesh.shape["pts"], ngrp=mesh.shape["grp"])
    return jax.shard_map(body, mesh=mesh, in_specs=in_specs, out_specs=(spread, spread), check_vma=False)
```

```python
import functools

import jax
import jax.numpy as jnp
from jax import lax
from jax.experimental import pallas as pl
from jax.experimental.pallas import tpu as pltpu
from jax.sharding import PartitionSpec as P

AXES = ("pts", "grp")
DAMP = 1.0
LANES = 128
ROWS = 48
LOW_ROWS = 32
GROUP = 8
SCATTER = 8


def split3(value):
    high = value.astype(jnp.bfloat16)
    rest = value - high.astype(jnp.float32)
    mid = rest.astype(jnp.bfloat16)
    low = (rest - mid.astype(jnp.float32)).astype(jnp.bfloat16)
    return high, mid, low


def dot_nn(left, right):
    return lax.dot_general(left, right, (((1,), (0,)), ((), ())), preferred_element_type=jnp.float32)


def dot_nt(left, right):
    return lax.dot_general(left, right, (((1,), (1,)), ((), ())), preferred_element_type=jnp.float32)


def row_of(row_at, col_at):
    if row_at == 8 and col_at == 8:
        return 36
    if row_at == 8:
        return 40 + col_at
    if col_at == 8:
        return 40 + row_at
    gap = (col_at - row_at) % 8
    if gap > 4 or (gap == 4 and row_at >= 4):
        return 8 * ((row_at - col_at) % 8) + col_at
    return 8 * gap + row_at


def side_of(device):
    for shift in (8, 4, 2, 1):
        device = device ^ (device >> shift)
    return device & 1


def other_half(named, side, half):
    swapped = jnp.where(named < half, named + half, named - half)
    return jnp.where(side == 0, named, swapped)


def terms_kernel(
    pt_ref, res_ref, point_ref, named_ref, cam_hbm,
    mine_ref, theirs_ref, red_ref, last_ref, place_ref,
    cam_ref, dense_ref, product_ref, total_ref, edge_ref, corner_ref, keep_ref, where_ref, sem,
):
    tiles = point_ref.shape[0]
    pitch = dense_ref.shape[0] // 8
    half = mine_ref.shape[1]
    cams = 2 * half
    load = pltpu.make_async_copy(cam_hbm, cam_ref, sem)
    load.start()
    row = lax.broadcasted_iota(jnp.int32, (8, LANES), 0)
    where_ref[...] = (point_ref[...] - point_ref[0:1, 0:1]).astype(jnp.float32)
    place_ref[...] = other_half(named_ref[...], side_of(lax.axis_index(AXES)), half)
    one = jnp.ones((LANES, LANES), jnp.bfloat16)
    zero_one = jnp.zeros((LANES, LANES), jnp.bfloat16)
    all_columns = []
    all_points = []
    for start in range(0, tiles, GROUP):
        points = where_ref[start : start + GROUP, :]
        both_ids = jnp.concatenate([points, place_ref[start : start + GROUP, :].astype(jnp.float32)], 0)
        all_points.append(points.astype(jnp.int32))
        all_columns.append(jnp.transpose(both_ids).astype(jnp.int32).astype(jnp.int16))

    places = where_ref[...]
    turned = jnp.transpose(places)
    tile_at = lax.broadcasted_iota(jnp.int32, (tiles, tiles), 0)
    other = lax.broadcasted_iota(jnp.int32, (tiles, tiles), 1)
    before = (other < tile_at) & (turned[LANES - 1 : LANES, :] == places[:, 0:1])
    after = (other > tile_at) & (turned[0:1, :] == places[:, LANES - 1 : LANES])
    before = jnp.where(before, 1.0, 0.0).astype(jnp.bfloat16)
    after = jnp.where(after, 1.0, 0.0).astype(jnp.bfloat16)
    head_rows = jnp.where(places == places[:, 0:1], 1.0, 0.0)
    tail_rows = jnp.where(places == places[:, LANES - 1 : LANES], 1.0, 0.0)

    for tile in range(tiles):
        here = slice(tile * LANES, (tile + 1) * LANES)
        dense_ref[pl.ds(tile, 8, stride=pitch), :] = jnp.concatenate([pt_ref[:, here], res_ref[:, here]], 0)
    entries = []
    for start in range(0, tiles, 8):
        top0, top1, top2, low0, low1, low2, res0, res1 = [
            dense_ref[pos * pitch + start : pos * pitch + start + 8, :] for pos in range(8)
        ]
        products = {
            0: top0 * top0 + low0 * low0,
            1: top1 * top1 + low1 * low1,
            2: top2 * top2 + low2 * low2,
            3: top0 * top1 + low0 * low1,
            4: top1 * top2 + low1 * low2,
            5: top0 * top2 + low0 * low2,
            8: top0 * res0 + low0 * res1,
            9: top1 * res0 + low1 * res1,
            10: top2 * res0 + low2 * res1,
        }
        entries.append(products)
        for pos in range(16):
            product_ref[pos * pitch + start : pos * pitch + start + 8, :] = products.get(pos, products[0])

    def gather(tile):
        columns = all_columns[tile // GROUP]
        at = tile % GROUP
        line = jnp.broadcast_to(all_points[tile // GROUP][at : at + 1], (16, LANES)).astype(jnp.int16)
        same = jnp.where(
            jnp.broadcast_to(columns[:, at : at + 1], (LANES, LANES)) == jnp.concatenate([line] * 8, 0),
            one,
            zero_one,
        )
        upper = product_ref[pl.ds(tile, 8, stride=pitch), :]
        lower = product_ref[pl.ds(8 * pitch + tile, 8, stride=pitch), :]
        left = jnp.concatenate(split3(jnp.concatenate([upper, lower], 0)), 0)
        found = dot_nn(left, same)
        found = found[0:16] + found[16:32] + found[32:48]
        total_ref[pl.ds(tile, 8, stride=pitch), :] = found[0:8]
        total_ref[pl.ds(8 * pitch + tile, 8, stride=pitch), :] = found[8:16]

    for tile in range(tiles // 2):
        gather(tile)

    lane8 = lax.broadcasted_iota(jnp.int32, (8, LANES), 1)
    heads = []
    tails = []
    for start in range(0, tiles, 8):
        head = jnp.zeros((8, LANES), jnp.float32)
        tail = jnp.zeros((8, LANES), jnp.float32)
        is_head = head_rows[start : start + 8]
        is_tail = tail_rows[start : start + 8]
        for pos, value in entries[start // 8].items():
            head = jnp.where(lane8 == pos, jnp.sum(value * is_head, axis=1, keepdims=True), head)
            tail = jnp.where(lane8 == pos, jnp.sum(value * is_tail, axis=1, keepdims=True), tail)
        heads.append(head)
        tails.append(tail)

    def carried(matrix, rows):
        parts = [dot_nn(matrix, part) for part in split3(jnp.concatenate(rows, 0))]
        return parts[0] + parts[1] + parts[2]

    from_before = carried(before, tails)
    from_after = carried(after, heads)

    for tile in range(tiles // 2, tiles):
        gather(tile)

    for start in range(0, tiles, 8):
        is_head = head_rows[start : start + 8]
        is_tail = tail_rows[start : start + 8]
        add_before = from_before[start : start + 8]
        add_after = from_after[start : start + 8]

        def total(pos):
            value = total_ref[pos * pitch + start : pos * pitch + start + 8, :]
            return value + is_head * add_before[:, pos : pos + 1] + is_tail * add_after[:, pos : pos + 1]

        v00, v11, v22 = [total(pos) + DAMP for pos in (0, 1, 2)]
        v01, v12, v02 = [total(pos) for pos in (3, 4, 5)]
        bees = [total(pos) for pos in (8, 9, 10)]
        dense = [dense_ref[pos * pitch + start : pos * pitch + start + 8, :] for pos in range(8)]
        c00 = v11 * v22 - v12 * v12
        c01 = v02 * v12 - v01 * v22
        c02 = v01 * v12 - v02 * v11
        c11 = v00 * v22 - v02 * v02
        c12 = v01 * v02 - v00 * v12
        c22 = v00 * v11 - v01 * v01
        scale = 1.0 / (v00 * c00 + v01 * c01 + v02 * c02)
        vinv = [[c00 * scale, c01 * scale, c02 * scale]]
        vinv.append([vinv[0][1], c11 * scale, c12 * scale])
        vinv.append([vinv[0][2], vinv[1][2], c22 * scale])

        def times(vec):
            return [vinv[at][0] * vec[0] + vinv[at][1] * vec[1] + vinv[at][2] * vec[2] for at in range(3)]

        def inner(left, right):
            return left[0] * right[0] + left[1] * right[1] + left[2] * right[2]

        top, low = dense[0:3], dense[3:6]
        use_top, use_low, weight = times(top), times(low), times(bees)
        results = (
            1.0 - inner(top, use_top),
            -inner(top, use_low),
            1.0 - inner(low, use_low),
            dense[6] - inner(top, weight),
            dense[7] - inner(low, weight),
        )
        for pos, value in enumerate(results):
            keep_ref[pos * tiles + start : pos * tiles + start + 8, :] = value

    load.wait()
    for tile in range(tiles):
        here = slice(tile * LANES, (tile + 1) * LANES)
        edge_ref[pl.ds(tile, 8, stride=pitch), :] = cam_ref[8:16, here]
        edge_ref[pl.ds(8 * pitch + tile, 2, stride=pitch), :] = cam_ref[16:18, here]
    for start in range(0, tiles, 8):
        here = slice(start, start + 8)
        zero8 = edge_ref[here, :]
        one8 = edge_ref[9 * pitch + start : 9 * pitch + start + 8, :]
        k00, k01, k11, s0, s1 = [keep_ref[pos * tiles + start : pos * tiles + start + 8, :] for pos in range(5)]
        corner_ref[here, :] = zero8 * (k00 * zero8 + k01 * one8) + one8 * (k01 * zero8 + k11 * one8)
        last_ref[here, :] = zero8 * s0 + one8 * s1
    lane16 = lax.broadcasted_iota(jnp.int32, (16, LANES), 1)
    names = [(lane16 + at * LANES).astype(jnp.int16) for at in range(cams // LANES)]
    one = jnp.ones((16, LANES), jnp.bfloat16)
    zero_one = jnp.zeros((16, LANES), jnp.bfloat16)
    acc = jnp.zeros((2 * ROWS + LOW_ROWS, cams), jnp.float32)
    for start in range(0, tiles, SCATTER):
        lefts = []
        rights = []
        for tile in range(start, start + SCATTER):
            here = slice(tile * LANES, (tile + 1) * LANES)

            def spread(ref, at):
                return ref[pl.ds(at, 8, stride=0), :]

            k00, k01, k11, s0, s1 = [spread(keep_ref, pos * tiles + tile) for pos in range(5)]
            zero = cam_ref[0:8, here]
            one_row = edge_ref[pl.ds(pitch + tile, 8, stride=pitch), :]
            zero8 = spread(edge_ref, tile)
            one8 = spread(edge_ref, 9 * pitch + tile)
            m0 = k00 * zero + k01 * one_row
            m1 = k01 * zero + k11 * one_row
            corner = spread(corner_ref, tile)
            pieces = [zero * m0 + one_row * m1]
            for gap in range(1, 5):
                pieces.append(zero * pltpu.roll(m0, 8 - gap, 0) + one_row * pltpu.roll(m1, 8 - gap, 0))
            pieces[4] = jnp.where(row == 4, corner, pieces[4])
            pieces.append(zero8 * m0 + one8 * m1)
            high, mid, low = split3(jnp.concatenate(pieces, 0))
            lefts.append(jnp.concatenate([high, mid, low[0:LOW_ROWS]], 0))
            red_ref[:, here] = zero * s0 + one_row * s1
            source = all_columns[tile // GROUP]
            column_at = GROUP + tile % GROUP
            for at in range(0, LANES, 16):
                column = jnp.broadcast_to(source[at : at + 16, column_at : column_at + 1], (16, LANES))
                rights.append(jnp.concatenate([jnp.where(column == name, one, zero_one) for name in names], 1))
        acc = acc + dot_nn(jnp.concatenate(lefts, 1), jnp.concatenate(rights, 0))
    low = jnp.concatenate([acc[2 * ROWS :], jnp.zeros((ROWS - LOW_ROWS, cams), jnp.float32)], 0)
    done = acc[0:ROWS] + acc[ROWS : 2 * ROWS] + low
    mine_ref[...] = done[:, 0:half]
    theirs_ref[...] = done[:, half:cams]


def inverse_of(entry):
    entry = dict(entry)
    root = {}
    factor = {}
    for col_at in range(9):
        root[col_at] = lax.rsqrt(entry[col_at, col_at])
        for row_at in range(col_at + 1, 9):
            factor[row_at, col_at] = entry[row_at, col_at] * root[col_at]
        for row_at in range(col_at + 1, 9):
            for inner in range(col_at + 1, row_at + 1):
                entry[row_at, inner] = entry[row_at, inner] - factor[row_at, col_at] * factor[inner, col_at]
    solved = {}
    for col_at in range(9):
        solved[col_at, col_at] = root[col_at]
        for row_at in range(col_at + 1, 9):
            value = factor[row_at, col_at] * solved[col_at, col_at]
            for inner in range(col_at + 1, row_at):
                value = value + factor[row_at, inner] * solved[inner, col_at]
            solved[row_at, col_at] = -value * root[row_at]
    result = {}
    for row_at in range(9):
        for col_at in range(row_at + 1):
            value = solved[row_at, row_at] * solved[row_at, col_at]
            for inner in range(row_at + 1, 9):
                value = value + solved[inner, row_at] * solved[inner, col_at]
            result[row_at, col_at] = value
    return result


def inverse_table(source_ref, entry_ref):
    half = source_ref.shape[1]
    cols = half // LANES
    step_rows = entry_ref.shape[0] // ROWS
    for block in range(ROWS // 8):
        for col in range(cols):
            entry_ref[pl.ds(block * 8 * step_rows + col, 8, stride=step_rows), :] = source_ref[
                block * 8 : block * 8 + 8, col * LANES : (col + 1) * LANES
            ]

    def entry_at(row_at, col_at):
        at = row_of(row_at, col_at) * step_rows
        return entry_ref[at : at + cols, :]

    entry = {(r, c): entry_at(r, c) for r in range(9) for c in range(r + 1)}
    for at in range(9):
        entry[at, at] = entry[at, at] + DAMP
    result = inverse_of(entry)
    spare = jnp.zeros((cols, LANES), jnp.float32)
    for at in (37, 38, 39):
        entry_ref[at * step_rows : at * step_rows + cols, :] = spare
    for (row_at, col_at), value in result.items():
        at = row_of(row_at, col_at) * step_rows
        entry_ref[at : at + cols, :] = value
    tables = []
    for col in range(cols):
        blocks = [
            entry_ref[pl.ds(block * 8 * step_rows + col, 8, stride=step_rows), :] for block in range(ROWS // 8)
        ]
        tables.append(jnp.concatenate(split3(jnp.concatenate(blocks, 0)), 0))
    return jnp.concatenate(tables, 1)


def add_parts(found):
    return found[0:ROWS] + found[ROWS : 2 * ROWS] + found[2 * ROWS : 3 * ROWS]


def owned_columns(table, slot_ref, at, owned):
    want = lax.broadcasted_iota(jnp.int32, (LANES, slot_ref.shape[1]), 0) + lax.axis_index(AXES) * owned
    pick = jnp.where(slot_ref[pl.ds(at, 1), :] == want, 1.0, 0.0).astype(jnp.bfloat16)
    return add_parts(dot_nt(table, pick))


def applied(table, place_ref, red_ref, last_ref, first, start):
    half = table.shape[1]
    row = lax.broadcasted_iota(jnp.int32, (8, LANES), 0)
    row16 = lax.broadcasted_iota(jnp.int32, (16, LANES), 0) + first
    one = jnp.ones((16, LANES), jnp.bfloat16)
    zero_one = jnp.zeros((16, LANES), jnp.bfloat16)
    rights = []
    for tile in range(start, start + GROUP):
        gap = (place_ref[pl.ds(tile, 16, stride=0), :] - row16).astype(jnp.int16)
        rights.append(
            jnp.concatenate([jnp.where(gap == jnp.int16(at), one, zero_one) for at in range(0, half, 16)], 0)
        )
    found = add_parts(dot_nn(table, jnp.concatenate(rights, 1)))
    results = []
    for at in range(GROUP):
        tile = start + at
        here = slice(tile * LANES, (tile + 1) * LANES)
        block = [found[8 * pos : 8 * pos + 8, at * LANES : (at + 1) * LANES] for pos in range(6)]
        red = red_ref[:, here]
        last = last_ref[pl.ds(tile, 8, stride=0), :]
        whole = jnp.where(row < 4, block[4], pltpu.roll(block[4], 4, 0))
        value = block[0] * red + block[5] * last + whole * pltpu.roll(red, 4, 0)
        for gap in range(1, 4):
            value = value + block[gap] * pltpu.roll(red, 8 - gap, 0)
            value = value + pltpu.roll(block[gap] * red, gap, 0)
        edge = jnp.sum(block[5] * red, axis=0, keepdims=True)
        results.append((tile, here, value, edge + (block[4] * last)[4:5]))
    return results


def first_half_kernel(
    mine_ref, place_ref, red_ref, last_ref, slot_ref,
    own_ref, part_ref, edge_ref,
    entry_ref, *, owned,
):
    table = inverse_table(mine_ref, entry_ref)
    for start in range(0, place_ref.shape[0], GROUP):
        for tile, here, value, edge in applied(table, place_ref, red_ref, last_ref, 0, start):
            part_ref[:, here] = value
            edge_ref[tile : tile + 1, :] = edge
    own_ref[...] = owned_columns(table, slot_ref, side_of(lax.axis_index(AXES)), owned)


def second_half_kernel(
    theirs_ref, place_ref, red_ref, last_ref, slot_ref, own_ref, part_ref, edge_ref,
    inv_hbm, out_hbm,
    entry_ref, square_ref, turned_ref, out_ref, sems, own_sem,
):
    tiles, half = place_ref.shape[0], theirs_ref.shape[1]
    owned = inv_hbm.shape[0]
    table = inverse_table(theirs_ref, entry_ref)
    own = own_ref[...] + owned_columns(table, slot_ref, 1 - side_of(lax.axis_index(AXES)), owned)
    square_ref[81:LANES, :] = jnp.zeros((LANES - 81, LANES), jnp.float32)
    for row_at in range(9):
        for col_at in range(9):
            at = row_of(row_at, col_at)
            square_ref[row_at * 9 + col_at : row_at * 9 + col_at + 1, :] = own[at : at + 1]
    turned_ref[...] = jnp.transpose(square_ref[...])[0:owned, 0:81]
    own_copy = pltpu.make_async_copy(turned_ref, inv_hbm, own_sem)
    own_copy.start()
    copies = []
    for start in range(0, tiles, GROUP):
        for tile, here, value, edge in applied(table, place_ref, red_ref, last_ref, half, start):
            out_ref[0:8, here] = value + part_ref[:, here]
            out_ref[8:9, here] = edge + edge_ref[tile : tile + 1, :]
        span = pl.ds(start * LANES, GROUP * LANES)
        copy = pltpu.make_async_copy(out_ref.at[:, span], out_hbm.at[:, span], sems.at[start // GROUP])
        copy.start()
        copies.append(copy)
    own_copy.wait()
    for copy in copies:
        copy.wait()


def partners(count, ngrp, masks):
    pairs = []
    for at in range(count):
        mask = masks[at.bit_count() % 2]
        pairs.append((at, at ^ (mask * ngrp + mask.bit_count() % 2)))
    return pairs


def exchange_steps(npts):
    bits = [1 << at for at in range(npts.bit_length() - 1)]
    pairs = [(bits[at], bits[at + 1], bits[at] + bits[at + 1]) for at in range(0, len(bits) - 1, 2)]
    turned = pairs[1:] + pairs[:1]
    steps = [list(zip(one, two)) for one, two in zip(pairs, turned)]
    if len(bits) % 2 == 1:
        steps.append([(bits[-1], bits[-1])])
    return steps


def shards(cam_jac, pt_jac, resid, obs_point, obs_camera, camera_slot, *, npts, ngrp):
    count = npts * ngrp
    cams = camera_slot.shape[0]
    half = cams // 2
    owned = cams // count
    size = obs_point.shape[0]
    tiles = size // LANES
    vmem = pl.BlockSpec(memory_space=pltpu.VMEM)
    hbm = pl.BlockSpec(memory_space=pl.ANY)

    def near(value):
        return pltpu.with_memory_space_constraint(value, pltpu.VMEM)

    mine, theirs, red, last, place = pl.pallas_call(
        terms_kernel,
        in_specs=[vmem] * 4 + [hbm],
        out_specs=[vmem] * 5,
        out_shape=[
            pltpu.VMEM((ROWS, half), jnp.float32),
            pltpu.VMEM((ROWS, half), jnp.float32),
            pltpu.VMEM((8, size), jnp.float32),
            pltpu.VMEM((tiles, LANES), jnp.float32),
            pltpu.VMEM((tiles, LANES), jnp.int32),
        ],
        scratch_shapes=[
            pltpu.VMEM(cam_jac.shape, jnp.float32),
            pltpu.VMEM((8 * (tiles + 8), LANES), jnp.float32),
            pltpu.VMEM((16 * (tiles + 8), LANES), jnp.float32),
            pltpu.VMEM((16 * (tiles + 8), LANES), jnp.float32),
            pltpu.VMEM((10 * (tiles + 8), LANES), jnp.float32),
            pltpu.VMEM((tiles, LANES), jnp.float32),
            pltpu.VMEM((5 * tiles, LANES), jnp.float32),
            pltpu.VMEM((tiles, LANES), jnp.float32),
            pltpu.SemaphoreType.DMA,
        ],
        name="terms",
    )(pt_jac, resid, obs_point.reshape(tiles, LANES), obs_camera.reshape(tiles, LANES), cam_jac)

    mate = [(at, at ^ 1) for at in range(count)]
    total = mine + lax.ppermute(theirs, AXES, mate)
    for step in exchange_steps(npts):
        got = [lax.ppermute(total, AXES, partners(count, ngrp, masks)) for masks in step]
        for value in got:
            total = total + value
    theirs = lax.ppermute(total, AXES, mate)

    place, red, last = near(place), near(red), near(last)
    slots = near(camera_slot.reshape(2, half))
    entries = pltpu.VMEM((ROWS * max(8, half // LANES), LANES), jnp.float32)
    own, part, edge = pl.pallas_call(
        functools.partial(first_half_kernel, owned=owned),
        in_specs=[vmem] * 5,
        out_specs=[vmem] * 3,
        out_shape=[
            pltpu.VMEM((ROWS, LANES), jnp.float32),
            pltpu.VMEM((8, size), jnp.float32),
            pltpu.VMEM((tiles, LANES), jnp.float32),
        ],
        scratch_shapes=[entries],
        name="apply_first",
    )(near(total), place, red, last, slots)
    inverse, precond = pl.pallas_call(
        second_half_kernel,
        in_specs=[vmem] * 8,
        out_specs=[hbm, hbm],
        out_shape=[
            jax.ShapeDtypeStruct((owned, 81), jnp.float32),
            jax.ShapeDtypeStruct((9, size), jnp.float32),
        ],
        scratch_shapes=[
            entries,
            pltpu.VMEM((LANES, LANES), jnp.float32),
            pltpu.VMEM((owned, 81), jnp.float32),
            pltpu.VMEM((9, size), jnp.float32),
            pltpu.SemaphoreType.DMA((tiles // GROUP,)),
            pltpu.SemaphoreType.DMA,
        ],
        name="apply_second",
    )(near(theirs), place, red, last, slots, near(own), near(part), near(edge))
    return (inverse.T, precond)


def solution(mesh):
    spread = P(None, AXES)
    in_specs = (spread, spread, spread, P(AXES), P(AXES), P())
    body = functools.partial(shards, npts=mesh.shape["pts"], ngrp=mesh.shape["grp"])
    return jax.shard_map(body, mesh=mesh, in_specs=in_specs, out_specs=(spread, spread), check_vma=False)
```
